32 devices in a mesh: groups: 2 (over y), seq: 4 (over z), batch: 2 (over x), head: 2 (over core).
Axes of the slice: x: 2, y: 2, z: 4, core: 2. Of those that a mesh axis runs over, the one named last changes fastest.
Arguments:
- hidden_in: bfloat16 [64, 4096], P(('groups', 'batch'), 'seq'), parts along dimension 0, may hold values from -400 to 400
- norm_gain_vector: bfloat16 [4096], P('seq'), may hold values from 0.099609375 to 1.8984375
- w_query: bfloat16 [4096, 4096], P('seq', 'head'), may hold values from -0.09375 to 0.09375
- key_cache_rows: bfloat16 [64, 4096, 128], P(('groups', 'batch'), 'seq'), parts along dimension 0, may hold values from -360 to 360
- value_cache_rows: bfloat16 [64, 4096, 128], P(('groups', 'batch'), 'seq'), parts along dimension 0, may hold values from -6 to 6
- k_new: bfloat16 [64, 128], P(('groups', 'batch')), parts along dimension 0, may hold values from -360 to 360
- v_new: bfloat16 [64, 128], P(('groups', 'batch')), parts along dimension 0, may hold values from -6 to 6
- lengths: int32 [64], P(('groups', 'batch')), parts along dimension 0, may hold values from 1 to 4096, as said below
- w_out: bfloat16 [4096, 4096], P('head', 'seq'), may hold values from -0.09375 to 0.09375
Outputs:
- layer_out: float32 [64, 4096], P(('groups', 'batch'), ('seq', 'head')), parts along dimension 0
The draws below stay inside these ranges and needn't reach their ends.
There are 2 independent parts, one for each index of `groups`. The reference program is written for one: setup_inputs(seed, part) draws one part's arguments, and reference() takes and returns one part's arrays. A program takes and returns all parts, laid end to end along the dimension named above; an argument that names none is the same for every part. Nothing has to cross between parts.
Inputs may be any that keep to these rules, and one draw needn't show every extreme that they name: `lengths`: every sequence has at least one cached position; some sequence of each draw uses all 4096.
All inputs are finite; a program needn't handle non-finite values.
Results may differ from the reference program's by a relative error of at most 0.008.
Values sent between devices are 32-bit elements; how exact they have to be, the bound alone decides.
A program may use at most 64 MiB of HBM per device.

```python
import jax
import jax.numpy as jnp
from jax import lax

D = 4096
HQ = 32
HD = 128
B = 32
CTX = 4096
QW = 4096


def drawn_keys(key, shape):
    values = jnp.clip(jax.random.normal(key, shape, jnp.float32), -6.0, 6.0) * 2.5
    return values


def draw_key_cache_rows(key, part):
    values = drawn_keys(jax.random.fold_in(key, 1), (B, CTX, HD))
    return values.astype(jnp.bfloat16)


def draw_k_new(key, part):
    values = drawn_keys(jax.random.fold_in(key, 2), (B, HD))
    return values.astype(jnp.bfloat16)


def draw_hidden_in(key, part):
    first, second, third = jax.random.split(jax.random.fold_in(key, 3), 3)
    base = jnp.clip(jax.random.normal(first, (B, D), jnp.float32), -4.0, 4.0)
    row_scale = jnp.exp(jax.random.uniform(second, (B, 1), jnp.float32) * jnp.log(10.0))
    ramp = jnp.arange(D, dtype=jnp.float32)[None, :] / D
    power = 0.24 * ramp + 0.76 * jax.random.uniform(third, (1, D), jnp.float32)
    col_scale = jnp.exp(power * jnp.log(10.0))
    return (base * row_scale * col_scale).astype(jnp.bfloat16)


def draw_lengths(key, part):
    first, second = jax.random.split(jax.random.fold_in(key, 4))
    values = jax.random.randint(first, (B,), 1, CTX + 1, jnp.int32)
    chosen = jax.random.randint(second, (), 0, B, jnp.int32)
    return jnp.where(jnp.arange(B, dtype=jnp.int32) == chosen, CTX, values).astype(jnp.int32)


def block_scale(stream_key, extent, cuts, least, top_value):
    level = 1.0
    for dim, blocks in cuts:
        steps = jax.random.uniform(jax.random.fold_in(jax.random.fold_in(stream_key, 6), dim), (blocks,), jnp.float32, least / len(cuts), top_value / len(cuts))
        level = level * jnp.repeat(jnp.exp(steps), extent[dim] // blocks).reshape((-1,) + (1,) * (len(extent) - 1 - dim))
    return level


def bell_draw(key, shape, scale, limit, shards=(), kind=jnp.bfloat16):
    gain = block_scale(key, shape, shards, -0.22, 0.18) if shards else 1.0
    entries = jax.random.normal(key, shape, jnp.float32) * scale * gain
    return jnp.minimum(jnp.maximum(entries, -limit), limit).astype(kind)


def setup_inputs(seed: int = 0, part: int = 0) -> dict:
    key_list = jax.random.split(jax.random.key(seed), 10)
    part_keys = jax.random.split(jax.random.fold_in(key_list[9], part), 10)
    hidden_in = draw_hidden_in(jax.random.fold_in(jax.random.fold_in(key_list[9], part), 71), part)
    norm_gain_vector = jnp.clip(1.0 + 0.18 * jax.random.normal(key_list[1], (D,), jnp.float32), 0.099609375, 1.8984375).astype(jnp.bfloat16)
    w_query = bell_draw(key_list[2], (D, QW), D ** -0.5, 0.09375, ((0, 4), (1, 2)))
    key_cache_rows = draw_key_cache_rows(jax.random.fold_in(jax.random.fold_in(key_list[9], part), 71), part)
    value_cache_rows = bell_draw(part_keys[4], (B, CTX, HD), 1.0, 6.0, ((0, 2), (1, 4)))
    k_new = draw_k_new(jax.random.fold_in(jax.random.fold_in(key_list[9], part), 71), part)
    v_new = bell_draw(part_keys[6], (B, HD), 1.0, 6.0, ((0, 2),))
    lengths = draw_lengths(jax.random.fold_in(jax.random.fold_in(key_list[9], part), 71), part)
    w_out = bell_draw(key_list[8], (QW, D), QW ** -0.5, 0.09375, ((0, 2), (1, 4)))
    return dict(hidden_in=hidden_in, norm_gain_vector=norm_gain_vector, w_query=w_query, key_cache_rows=key_cache_rows, value_cache_rows=value_cache_rows, k_new=k_new, v_new=v_new, lengths=lengths, w_out=w_out)


def reference(hidden_in, norm_gain_vector, w_query, key_cache_rows, value_cache_rows, k_new, v_new, lengths, w_out):
    inputs = hidden_in.astype(jnp.float32)
    mean_sq = lax.optimization_barrier(jnp.mean(inputs * inputs, axis=-1, keepdims=True))
    normed = (inputs * lax.rsqrt(mean_sq + 1e-05) * norm_gain_vector.astype(jnp.float32)).astype(jnp.bfloat16)
    inverse_root_norm = 1.0 / HD ** 0.5
    query_vectors = (jnp.dot(normed, w_query, preferred_element_type=jnp.float32) * inverse_root_norm).astype(jnp.bfloat16)
    query_vectors = query_vectors.reshape(query_vectors.shape[0], HQ, HD)

    def attend(per_seq):
        query_rows, key_rows, value_rows, used, key_own, value_own = per_seq
        scores = jnp.dot(query_rows, key_rows.T, preferred_element_type=jnp.float32)
        own = jnp.dot(query_rows, key_own, preferred_element_type=jnp.float32)
        live_mask = lax.iota(jnp.int32, key_rows.shape[0]) < used
        top = jnp.maximum(lax.optimization_barrier(jnp.max(jnp.where(live_mask[None, :], scores, -jnp.inf), axis=-1)), own)
        softmax_weights = jnp.where(live_mask[None, :], jnp.exp(scores - top[:, None]), jnp.float32(0.0))
        fresh = jnp.exp(own - top)
        totals = lax.optimization_barrier(jnp.sum(softmax_weights, axis=-1)) + fresh
        summed = jnp.dot(softmax_weights.astype(jnp.bfloat16), value_rows, preferred_element_type=jnp.float32)
        result = (summed + fresh[:, None] * value_own.astype(jnp.float32)[None, :]) / totals[:, None]
        return result.astype(jnp.bfloat16).reshape(HQ * HD)
    attended = lax.map(attend, (query_vectors, key_cache_rows, value_cache_rows, lengths, k_new, v_new))
    return jnp.dot(attended, w_out, preferred_element_type=jnp.float32)
```

```python
import functools

import jax
import jax.numpy as jnp
from jax import lax
from jax.experimental import pallas as pl
from jax.experimental.pallas import tpu as pltpu
from jax.sharding import PartitionSpec as P

HD = 128
EPS = 1e-05
MESH = pl.DeviceIdType.MESH
F32 = jnp.float32
BF16 = jnp.bfloat16


def chunk_edges(heads, cuts):
    step = heads // cuts
    return [(c * step, (c + 1) * step) for c in range(cuts)]


def kernel(
    n,
    heads,
    rows,
    cuts,
    m,
    subs,
    lens_hbm,
    hidden_hbm,
    gain_hbm,
    wq_hbm,
    keys_hbm,
    values_hbm,
    knew_hbm,
    vnew_hbm,
    wout_hbm,
    out_ref,
    lens_ref,
    hid,
    gain,
    wq,
    kbuf,
    vbuf,
    knew,
    vnew,
    wout,
    newf,
    qsend,
    qrecv,
    qturn,
    qall,
    asend,
    arecv,
    att,
    hsend,
    hrecv,
    small_sem,
    wq_sem,
    k_sem,
    v_sem,
    wo_sem,
    qs_send,
    qs_recv,
    qg_send,
    qg_recv,
    as_send,
    as_recv,
    ag_send,
    ag_recv,
    h_send,
    h_recv,
):
    me = lax.axis_index("seq")
    core = lax.axis_index("head")
    other = 1 - core
    first = (n - m) // 2
    share = rows // m
    piece = share // subs
    block = keys_hbm.shape[1]
    width = wq_hbm.shape[0] * n
    edges = chunk_edges(heads, cuts)
    owning = jnp.logical_and(me >= first, me < first + m)
    my_slot = jnp.clip(me - first, 0, m - 1)
    slots = [lax.rem(my_slot + k, m) for k in range(m)]
    away = [(n // 2 + k) % n for k in range(n)]
    away = [k for k in away if k]

    barrier = pltpu.get_barrier_semaphore()

    def greet(s):
        pl.semaphore_signal(
            barrier, inc=1, device_id={"seq": s, "head": core}, device_id_type=MESH
        )

    for s in range(n):
        meet = me != s
        if not first <= s < first + m:
            meet = jnp.logical_and(meet, owning)
        pl.when(meet)(functools.partial(greet, s))
    pl.semaphore_signal(barrier, inc=1, device_id={"head": other}, device_id_type=MESH)

    small = [
        pltpu.make_async_copy(src, dst, small_sem.at[i])
        for i, (src, dst) in enumerate(
            (
                (hidden_hbm, hid),
                (gain_hbm, gain),
                (knew_hbm, knew),
                (vnew_hbm, vnew),
                (lens_hbm, lens_ref),
            )
        )
    ]
    for copy in small[:2]:
        copy.start()
    wq_copies = []
    for c, (lo, hi) in enumerate(edges):
        cols = pl.ds(lo * HD, (hi - lo) * HD)
        wq_copies.append(pltpu.make_async_copy(wq_hbm.at[:, cols], wq.at[:, cols], wq_sem.at[c]))
        wq_copies[-1].start()
    for copy in small[2:]:
        copy.start()
    k_copies, v_copies = [], []
    for k in range(m):
        group = pl.ds(slots[k] * share, share)
        k_copies.append(pltpu.make_async_copy(keys_hbm.at[group], kbuf.at[k], k_sem.at[k]))
        v_copies.append(pltpu.make_async_copy(values_hbm.at[group], vbuf.at[k], v_sem.at[k]))
    half = wout_hbm.shape[1] // 2
    wo_copies = []
    for i, side in enumerate((other, core)):
        cols = pl.ds(pl.multiple_of(side * half, HD), half)
        wo_copies.append(pltpu.make_async_copy(wout_hbm.at[:, cols], wout.at[i], wo_sem.at[i]))

    small[0].wait()
    small[1].wait()
    x = hid[...].astype(F32)
    squares = jnp.sum(x * x, axis=-1, keepdims=True)
    g = gain[...].astype(F32)
    scaled = jnp.concatenate(
        [x[:, i * HD : (i + 1) * HD] * g[i : i + 1] for i in range(g.shape[0])], axis=1
    )
    upper = scaled.astype(BF16)
    lower = (scaled - upper.astype(F32)).astype(BF16)
    both = jnp.concatenate([upper, lower], axis=0)
    for p in range(m):
        qsend[p, 0] = jnp.broadcast_to(squares[p * share : (p + 1) * share], (share, HD))
    qs = [[None] * m for _ in edges]

    def arrivals(c, s):
        lo, hi = edges[c]
        span = pl.ds(0 if c == 0 else lo + 1, hi + 1 - (0 if c == 0 else lo + 1))
        return pltpu.make_async_remote_copy(
            src_ref=qsend.at[0, span],
            dst_ref=qrecv.at[s, span],
            send_sem=qs_send.at[c, 0],
            recv_sem=qs_recv.at[c, s],
            device_id={"seq": me, "head": core},
            device_id_type=MESH,
        )

    for c, (lo, hi) in enumerate(edges):
        wq_copies[c].wait()
        if c == cuts - 1:
            for copy in [x for pair in zip(k_copies, v_copies) for x in pair] + wo_copies:
                copy.start()
        product = jnp.dot(both, wq[:, lo * HD : hi * HD], preferred_element_type=F32)
        part = product[:rows] + product[rows:]
        for h in range(lo, hi):
            for p in range(m):
                qsend[p, h + 1] = part[
                    p * share : (p + 1) * share, (h - lo) * HD : (h - lo + 1) * HD
                ]
        if c == 0:
            pl.semaphore_wait(barrier, jnp.where(owning, n, m + 1))
        start = 0 if c == 0 else lo + 1
        span = pl.ds(start, hi + 1 - start)
        for k in reversed(range(m)):
            qs[c][k] = pltpu.make_async_remote_copy(
                src_ref=qsend.at[slots[k], span],
                dst_ref=qrecv.at[me, span],
                send_sem=qs_send.at[c, k],
                recv_sem=qs_recv.at[c, me],
                device_id={"seq": slots[k] + first, "head": core},
                device_id_type=MESH,
            )
            if k:
                qs[c][k].start()
            else:
                pl.when(jnp.logical_not(owning))(qs[c][k].start)

    for copy in small[2:]:
        copy.wait()
    newf[0] = knew[...].astype(F32)
    newf[1] = vnew[...].astype(F32)

    def gathers(u):
        return [
            pltpu.make_async_remote_copy(
                src_ref=qall.at[my_slot, pl.ds(u * piece, piece)],
                dst_ref=qall.at[my_slot, pl.ds(u * piece, piece)],
                send_sem=qg_send.at[u, i],
                recv_sem=qg_recv.at[u, my_slot],
                device_id={"seq": lax.rem(me + k, n), "head": core},
                device_id_type=MESH,
            )
            for i, k in enumerate(away)
        ]

    @pl.when(owning)
    def _():
        for c in range(len(edges)):
            for s in range(1, n):
                arrivals(c, lax.rem(me + s, n)).wait_recv()
        total = qsend[my_slot]
        for s in range(1, n):
            total = total + qrecv[lax.rem(me + s, n)]
        inv = lax.rsqrt(total[0] / width + EPS) * (1.0 / HD**0.5)
        qturn[...] = (total[1:] * inv[None]).astype(BF16).astype(F32)
        for u in range(subs):
            for r in range(u * piece, (u + 1) * piece):
                qall[my_slot, r] = qturn[:, r, :]
            for copy in gathers(u):
                copy.start()

    lanes = lax.broadcasted_iota(jnp.int32, (heads, HD), 1)
    positions = me * block + lax.broadcasted_iota(jnp.int32, (heads, block), 1)
    sends = []
    for k in range(m):
        for u in range(subs):
            i = k * subs + u
            arrival = pltpu.make_async_remote_copy(
                src_ref=qall.at[my_slot, pl.ds(u * piece, piece)],
                dst_ref=qall.at[slots[k], pl.ds(u * piece, piece)],
                send_sem=qg_send.at[u, 0],
                recv_sem=qg_recv.at[u, slots[k]],
                device_id={"seq": me, "head": core},
                device_id_type=MESH,
            )
            if k:
                arrival.wait_recv()
            else:
                pl.when(jnp.logical_not(owning))(arrival.wait_recv)
            if u == 0:
                k_copies[k].wait()
            scores, own = [], []
            for r in range(piece):
                q = qall[slots[k], u * piece + r]
                scores.append(
                    lax.dot_general(
                        q.astype(BF16),
                        kbuf[k, u * piece + r],
                        (((1,), (1,)), ((), ())),
                        preferred_element_type=F32,
                    )
                )
                row = slots[k] * share + u * piece + r
                own.append(jnp.sum(q * newf[0, pl.ds(row, 1)], axis=-1, keepdims=True))
            if u == 0:
                v_copies[k].wait()
            stats = jnp.zeros((heads, HD), F32)
            for r in range(piece):
                live = positions < lens_ref[slots[k] * share + u * piece + r]
                masked = jnp.where(live, scores[r], -jnp.inf)
                top = jnp.maximum(jnp.max(masked, axis=-1, keepdims=True), own[r])
                weights = jnp.exp(masked - top)
                weight = jnp.sum(weights, axis=-1, keepdims=True)
                stats = jnp.where(lanes == 2 * r, top, stats)
                stats = jnp.where(lanes == 2 * r + 1, weight, stats)
                asend[i, r] = jnp.dot(
                    weights.astype(BF16), vbuf[k, u * piece + r], preferred_element_type=F32
                )
            asend[i, piece] = stats
            sends.append(
                pltpu.make_async_remote_copy(
                    src_ref=asend.at[i],
                    dst_ref=arecv.at[me, u],
                    send_sem=as_send.at[i],
                    recv_sem=as_recv.at[u, me],
                    device_id={"seq": slots[k] + first, "head": core},
                    device_id_type=MESH,
                )
            )
            if k:
                sends[-1].start()
            else:
                pl.when(jnp.logical_not(owning))(sends[-1].start)

    def returns(u):
        return [
            pltpu.make_async_remote_copy(
                src_ref=att.at[pl.ds(my_slot * share + u * piece, piece)],
                dst_ref=att.at[pl.ds(my_slot * share + u * piece, piece)],
                send_sem=ag_send.at[u, i],
                recv_sem=ag_recv.at[u, my_slot],
                device_id={"seq": lax.rem(me + k, n), "head": core},
                device_id_type=MESH,
            )
            for i, k in enumerate(away)
        ]

    @pl.when(owning)
    def _():
        for u in range(subs):
            others = [lax.rem(me + s, n) for s in range(1, n)]
            for s in others:
                pltpu.make_async_remote_copy(
                    src_ref=asend.at[0],
                    dst_ref=arecv.at[s, u],
                    send_sem=as_send.at[0],
                    recv_sem=as_recv.at[u, s],
                    device_id={"seq": me, "head": core},
                    device_id_type=MESH,
                ).wait_recv()
            stats = [asend[u, piece]] + [arecv[s, u, piece] for s in others]
            for r in range(piece):
                row = my_slot * share + u * piece + r
                tops = [s[:, 2 * r : 2 * r + 1] for s in stats]
                own = jnp.sum(
                    qall[my_slot, u * piece + r] * newf[0, pl.ds(row, 1)], axis=-1, keepdims=True
                )
                top = functools.reduce(jnp.maximum, tops)
                fresh = jnp.exp(own - top)
                totals = fresh
                summed = fresh * newf[1, pl.ds(row, 1)]
                for s in range(n):
                    factor = jnp.exp(tops[s] - top)
                    totals = totals + stats[s][:, 2 * r + 1 : 2 * r + 2] * factor
                    summed = summed + (arecv[others[s - 1], u, r] if s else asend[u, r]) * factor
                att[row] = (summed / totals).astype(BF16).astype(F32)
            for copy in returns(u):
                copy.start()

    for copy in wo_copies:
        copy.wait()
    for j in range(m):
        for u in range(subs):
            group = pl.ds(j * share + u * piece, piece)
            arrival = pltpu.make_async_remote_copy(
                src_ref=att.at[group],
                dst_ref=att.at[group],
                send_sem=ag_send.at[u, 0],
                recv_sem=ag_recv.at[u, j],
                device_id={"seq": me, "head": core},
                device_id_type=MESH,
            )
            pl.when(me != first + j)(arrival.wait_recv)

    attended = jnp.concatenate([att[:, h, :] for h in range(heads)], axis=1).astype(BF16)
    hsend[...] = jnp.dot(attended, wout[0], preferred_element_type=F32)
    swap = pltpu.make_async_remote_copy(
        src_ref=hsend,
        dst_ref=hrecv,
        send_sem=h_send,
        recv_sem=h_recv,
        device_id={"head": other},
        device_id_type=MESH,
    )
    swap.start()
    kept = jnp.dot(attended, wout[1], preferred_element_type=F32)
    swap.wait_recv()
    out_ref[...] = kept + hrecv[...]

    for c in range(len(edges)):
        for k in range(1, m):
            qs[c][k].wait_send()
    for copy in sends[subs:]:
        copy.wait_send()
    swap.wait_send()

    @pl.when(owning)
    def _():
        for u in range(subs):
            for copy in gathers(u) + returns(u):
                copy.wait_send()

    @pl.when(jnp.logical_not(owning))
    def _():
        for c in range(len(edges)):
            qs[c][0].wait_send()
        for copy in sends[:subs]:
            copy.wait_send()


def solution(mesh):
    n = mesh.shape["seq"]
    cuts = 2
    m = max(n // 2, 1)
    subs = 2

    def shards(hidden, gain, wq, keys, values, knew, vnew, lengths, wout):
        rows, depth = hidden.shape
        heads = wq.shape[1] // HD
        share = rows // m
        piece = share // subs
        block = keys.shape[1]
        half = wout.shape[1] // 2
        anywhere = pl.BlockSpec(memory_space=pl.ANY)
        dma = pltpu.SemaphoreType.DMA
        return pl.pallas_call(
            functools.partial(kernel, n, heads, rows, cuts, m, subs),
            out_shape=pltpu.VMEM((rows, half), F32),
            in_specs=[anywhere] * 9,
            out_specs=pl.BlockSpec(memory_space=pltpu.VMEM),
            scratch_shapes=[
                pltpu.SMEM((rows,), jnp.int32),
                pltpu.VMEM((rows, depth), BF16),
                pltpu.VMEM((depth // HD, HD), BF16),
                pltpu.VMEM(wq.shape, BF16),
                pltpu.VMEM((m, share, block, HD), BF16),
                pltpu.VMEM((m, share, block, HD), BF16),
                pltpu.VMEM((rows, HD), BF16),
                pltpu.VMEM((rows, HD), BF16),
                pltpu.VMEM((2, wout.shape[0], half), BF16),
                pltpu.VMEM((2, rows, HD), F32),
                pltpu.VMEM((m, heads + 1, share, HD), F32),
                pltpu.VMEM((n, heads + 1, share, HD), F32),
                pltpu.VMEM((heads, share, HD), F32),
                pltpu.VMEM((m, share, heads, HD), F32),
                pltpu.VMEM((m * subs, piece + 1, heads, HD), F32),
                pltpu.VMEM((n, subs, piece + 1, heads, HD), F32),
                pltpu.VMEM((rows, heads, HD), F32),
                pltpu.VMEM((rows, half), F32),
                pltpu.VMEM((rows, half), F32),
                dma((5,)),
                dma((cuts,)),
                dma((m,)),
                dma((m,)),
                dma((2,)),
                dma((cuts, m)),
                dma((cuts, n)),
                dma((subs, n)),
                dma((subs, m)),
                dma((m * subs,)),
                dma((subs, n)),
                dma((subs, n)),
                dma((subs, m)),
                dma(()),
                dma(()),
            ],
            compiler_params=pltpu.CompilerParams(collective_id=0, has_side_effects=True),
            name="decode_step",
        )(lengths, hidden, gain.reshape(-1, HD), wq, keys, values, knew, vnew, wout)

    placed = (
        P(("groups", "batch"), "seq"),
        P("seq"),
        P("seq", "head"),
        P(("groups", "batch"), "seq", None),
        P(("groups", "batch"), "seq", None),
        P(("groups", "batch"), None),
        P(("groups", "batch"), None),
        P(("groups", "batch")),
        P("head", "seq"),
    )
    return jax.shard_map(
        shards,
        mesh=mesh,
        in_specs=placed,
        out_specs=P(("groups", "batch"), ("seq", "head")),
        check_vma=False,
    )
```

```python
import functools

import jax
import jax.numpy as jnp
from jax import lax
from jax.experimental import pallas as pl
from jax.experimental.pallas import tpu as pltpu
from jax.sharding import PartitionSpec as P

HD = 128
EPS = 1e-05
MESH = pl.DeviceIdType.MESH
F32 = jnp.float32
BF16 = jnp.bfloat16
CUTS = 4
CHUNKS = 2
FARFIRST = 0


def outside_in(n):
    order = []
    for k in range((n + 1) // 2):
        order += [k] if k == n - 1 - k else [k, n - 1 - k]
    return order


def kernel(
    n,
    heads,
    rows,
    m,
    cuts,
    chunks,
    lens_hbm,
    hidden_hbm,
    gain_hbm,
    wq_hbm,
    keys_hbm,
    values_hbm,
    knew_hbm,
    vnew_hbm,
    wout_hbm,
    out_ref,
    lens_ref,
    hid,
    gain,
    wq,
    kbuf,
    vbuf,
    newb,
    wout,
    newf,
    qsend,
    qrecv,
    qturn,
    qown,
    qall,
    asend,
    arecv,
    aout,
    att,
    hsend,
    hrecv,
    tally,
    in_sem,
    wq_sem,
    kv_sem,
    wo_sem,
    qs_send,
    qs_recv,
    qg_send,
    qg_recv,
    as_send,
    as_recv,
    ag_send,
    ag_recv,
    h_sem,
):
    me = lax.axis_index("seq")
    core = lax.axis_index("head")
    other = 1 - core
    first = (n - m) // 2
    share = rows // m
    piece = share // 2
    half_rows = rows // 2
    block = keys_hbm.shape[1]
    width = wq_hbm.shape[0] * n
    step = heads // cuts
    hc = heads // chunks
    full = 2 * hc
    per_chunk = cuts // chunks
    on_chip = jnp.logical_and(me >= first, me < first + m)
    owning = jnp.logical_and(on_chip, core == 1)
    resting = jnp.logical_not(owning)
    my_j = jnp.clip(me - first, 0, m - 1)
    order = outside_in(n)

    def device(z, h):
        return {"seq": z, "head": h}

    def is_me(z, h):
        return jnp.logical_and(me == z, core == h)

    def not_me(z, h):
        return jnp.logical_not(is_me(z, h))

    barrier = pltpu.get_barrier_semaphore()

    def greet(z, h):
        pl.semaphore_signal(barrier, inc=1, device_id=device(z, h), device_id_type=MESH)

    for z in order:
        for h in (0, 1):
            meet = not_me(z, h)
            if h == 0 or not first <= z < first + m:
                partner = jnp.logical_and(me == z, core == 1 - h)
                meet = jnp.logical_and(meet, jnp.logical_or(owning, partner))
            pl.when(meet)(functools.partial(greet, z, h))
    greeted = jnp.where(owning, 2 * n - 1, jnp.where(on_chip, m, m + 1))

    ins = [
        pltpu.make_async_copy(src, dst, in_sem.at[i])
        for i, src, dst in (
            (0, hidden_hbm, hid),
            (1, gain_hbm, gain),
            (2, knew_hbm, newb.at[0]),
            (2, vnew_hbm, newb.at[1]),
            (3, lens_hbm, lens_ref),
        )
    ]
    for copy in ins[:2]:
        copy.start()
    wq_copies = []
    for c in range(cuts):
        cols = pl.ds(c * step * HD, step * HD)
        wq_copies.append(pltpu.make_async_copy(wq_hbm.at[:, cols], wq.at[:, cols], wq_sem.at[c]))
        wq_copies[-1].start()
    for copy in ins[2:]:
        copy.start()
    group = pl.ds(core * half_rows, half_rows)
    half = wout_hbm.shape[1] // 2
    later = [
        pltpu.make_async_copy(keys_hbm.at[group], kbuf, kv_sem.at[0]),
        pltpu.make_async_copy(values_hbm.at[group], vbuf, kv_sem.at[1]),
    ]
    for i, side in enumerate((other, core)):
        cols = pl.ds(pl.multiple_of(side * half, HD), half)
        later.append(pltpu.make_async_copy(wout_hbm.at[:, cols], wout.at[i], wo_sem))

    ins[0].wait()
    ins[1].wait()
    x = hid[...].astype(F32)
    x = jnp.concatenate(
        [
            x[u * half_rows + j * piece : u * half_rows + (j + 1) * piece]
            for j in range(m)
            for u in (0, 1)
        ],
        axis=0,
    )
    squares = jnp.sum(x * x, axis=-1, keepdims=True)
    g = gain[...].astype(F32)
    scaled = jnp.concatenate(
        [x[:, i * HD : (i + 1) * HD] * g[i : i + 1] for i in range(g.shape[0])], axis=1
    )
    upper = scaled.astype(BF16)
    lower = (scaled - upper.astype(F32)).astype(BF16)
    both = jnp.concatenate([upper, lower], axis=0)
    for j in range(m):
        qsend[j, 0] = jnp.broadcast_to(squares[j * share : (j + 1) * share], (share, HD))

    def span(c):
        return pl.ds(0 if c == 0 else c * step + 1, step + (1 if c == 0 else 0))

    def partial_send(c, j):
        return pltpu.make_async_remote_copy(
            src_ref=qsend.at[j, span(c)],
            dst_ref=qrecv.at[2 * me + core, span(c)],
            send_sem=qs_send,
            recv_sem=qs_recv.at[c // per_chunk],
            device_id=device(first + j, 1),
            device_id_type=MESH,
        )

    def place_own(j, c):
        qrecv[2 * me + 1, span(c)] = qsend[j, span(c)]

    for c in range(cuts):
        wq_copies[c].wait()
        if c == cuts - 1:
            for copy in later:
                copy.start()
        product = jnp.dot(
            both, wq[:, c * step * HD : (c + 1) * step * HD], preferred_element_type=F32
        )
        part = product[:rows] + product[rows:]
        for h in range(step):
            for j in range(m):
                qsend[j, c * step + h + 1] = part[
                    j * share : (j + 1) * share, h * HD : (h + 1) * HD
                ]
        if c == 0:
            pl.semaphore_wait(barrier, greeted)
        for j in range(m):
            pl.when(not_me(first + j, 1))(partial_send(c, j).start)
            pl.when(is_me(first + j, 1))(functools.partial(place_own, j, c))

    pltpu.make_async_copy(newb, newb, in_sem.at[2]).wait()
    ins[4].wait()
    newf[...] = newb[...].astype(F32)

    def query_sends(c):
        return [
            (
                not_me(z, u),
                pltpu.make_async_remote_copy(
                    src_ref=qall.at[c, my_j] if u else qown.at[c],
                    dst_ref=qall.at[c, my_j],
                    send_sem=qg_send,
                    recv_sem=qg_recv.at[c, my_j],
                    device_id=device(z, u),
                    device_id_type=MESH,
                ),
            )
            for u in (0, 1)
            for z in order
        ]

    @pl.when(owning)
    def _():
        for c in range(chunks):
            lo = 0 if c == 0 else 1 + c * hc
            arrived = qrecv.at[pl.ds(0, 2 * n - 1), pl.ds(lo, 1 + (c + 1) * hc - lo)]
            pltpu.make_async_copy(arrived, arrived, qs_recv.at[c]).wait()
            total = functools.reduce(jnp.add, [qrecv[2 * z + 1, 0] for z in range(n)])
            inv = lax.rsqrt(total / width + EPS) * (1.0 / HD**0.5)
            for h in (0, 1):
                planes = pl.ds(1 + c * hc, hc)
                q = functools.reduce(jnp.add, [qrecv[2 * z + h, planes] for z in range(n)])
                qturn[h * hc : (h + 1) * hc] = (q * inv[None]).astype(BF16).astype(F32)
            for r in range(piece):
                qown[c, r] = qturn[:, r, :]
                qall[c, my_j, r] = qturn[:, piece + r, :]
            for go, copy in query_sends(c):
                pl.when(go)(copy.start)

    lanes = lax.broadcasted_iota(jnp.int32, (full, HD), 1)
    lanes = lanes - lax.broadcasted_iota(jnp.int32, (full, HD), 0) // 8 * (2 * piece)
    positions = me * block + lax.broadcasted_iota(jnp.int32, (full, block), 1)

    def keep_own(c):
        arecv[c, 1, me] = asend[c, my_j]

    def result_send(c, j):
        return pltpu.make_async_remote_copy(
            src_ref=asend.at[c, j],
            dst_ref=arecv.at[c, core, me],
            send_sem=as_send,
            recv_sem=as_recv.at[c, core],
            device_id=device(first + j, 1),
            device_id_type=MESH,
        )

    for c in range(chunks):
        for k in range(m):
            far = c == chunks - 1 and FARFIRST
            j = lax.rem(my_j + (m - 1 - k if far else k), m)
            arrival = pltpu.make_async_remote_copy(
                src_ref=qall.at[c, j],
                dst_ref=qall.at[c, j],
                send_sem=qg_send,
                recv_sem=qg_recv.at[c, j],
                device_id=device(me, other),
                device_id_type=MESH,
            )
            pl.when(not_me(first + j, 1))(arrival.wait_recv)
            if c == 0 and k == 0:
                later[0].wait()
            scores, own = [], []
            for r in range(piece):
                q = qall[c, j, r]
                scores.append(
                    lax.dot_general(
                        q.astype(BF16),
                        kbuf[j * piece + r],
                        (((1,), (1,)), ((), ())),
                        preferred_element_type=F32,
                    )
                )
                row = core * half_rows + j * piece + r
                own.append(jnp.sum(q * newf[0, pl.ds(row, 1)], axis=-1, keepdims=True))
            if c == 0 and k == 0:
                later[1].wait()
            stats = jnp.zeros((full, HD), F32)
            for r in range(piece):
                live = positions < lens_ref[core * half_rows + j * piece + r]
                masked = jnp.where(live, scores[r], -jnp.inf)
                top = jnp.maximum(jnp.max(masked, axis=-1, keepdims=True), own[r])
                weights = jnp.exp(masked - top)
                weight = jnp.sum(weights, axis=-1, keepdims=True)
                stats = jnp.where(lanes == 2 * r, top, stats)
                stats = jnp.where(lanes == 2 * r + 1, weight, stats)
                asend[c, j, r * full : (r + 1) * full] = jnp.dot(
                    weights.astype(BF16), vbuf[j * piece + r], preferred_element_type=F32
                )
            asend[c, j, piece * full : piece * full + 8] = functools.reduce(
                jnp.add, [stats[i : i + 8] for i in range(0, full, 8)]
            )
            pl.when(not_me(first + j, 1))(result_send(c, j).start)
            pl.when(is_me(first + j, 1))(functools.partial(keep_own, c))

    def returns(c, u):
        group = pl.ds(u * half_rows + my_j * piece, piece)
        return [
            (
                not_me(z, h),
                pltpu.make_async_remote_copy(
                    src_ref=att.at[c, group] if h else aout.at[c, u],
                    dst_ref=att.at[c, group],
                    send_sem=ag_send,
                    recv_sem=ag_recv.at[c],
                    device_id=device(z, h),
                    device_id_type=MESH,
                ),
            )
            for z in order
            for h in (0, 1)
        ]

    @pl.when(owning)
    def _():
        for c in range(chunks):
            for u in (1, 0):
                arrived = arecv.at[c, u, pl.ds(0, n - u)]
                pltpu.make_async_copy(arrived, arrived, as_recv.at[c, u]).wait()
                stats = [arecv[c, u, z, piece * full : piece * full + 8] for z in range(n)]
                for r in range(piece):
                    row = u * half_rows + my_j * piece + r

                    def column(s, i):
                        at = [2 * piece * t + 2 * r + i for t in range(full // 8)]
                        return jnp.concatenate([s[:, a : a + 1] for a in at], axis=0)

                    tops = [column(s, 0) for s in stats]
                    q = qall[c, my_j, r] if u else qown[c, r]
                    own = jnp.sum(q * newf[0, pl.ds(row, 1)], axis=-1, keepdims=True)
                    top = functools.reduce(jnp.maximum, tops)
                    fresh = jnp.exp(own - top)
                    totals = fresh
                    summed = fresh * newf[1, pl.ds(row, 1)]
                    for z in range(n):
                        factor = jnp.exp(tops[z] - top)
                        totals = totals + column(stats[z], 1) * factor
                        summed = summed + arecv[c, u, z, r * full : (r + 1) * full] * factor
                    result = (summed / totals).astype(BF16).astype(F32)
                    aout[c, u, r] = result[:hc]
                    att[c, row] = result[hc:]
                for go, copy in returns(c, u):
                    pl.when(go)(copy.start)

    sent, kept = None, None
    for c in range(chunks):
        for owner, count in ((owning, rows - share), (resting, rows)):
            arrived = att.at[c, pl.ds(0, count)]
            pl.when(owner)(pltpu.make_async_copy(arrived, arrived, ag_recv.at[c]).wait)
        if c == 0:
            pltpu.make_async_copy(wout, wout, wo_sem).wait()
        attended = jnp.concatenate([att[c, :, h, :] for h in range(hc)], axis=1).astype(BF16)
        deep = slice(c * hc * HD, (c + 1) * hc * HD)
        product = jnp.dot(attended, wout[0, deep], preferred_element_type=F32)
        sent = product if sent is None else sent + product
        if c == chunks - 1:
            hsend[...] = sent
            swap = pltpu.make_async_remote_copy(
                src_ref=hsend,
                dst_ref=hrecv,
                send_sem=h_sem.at[0],
                recv_sem=h_sem.at[1],
                device_id=device(me, other),
                device_id_type=MESH,
            )
            swap.start()
        product = jnp.dot(attended, wout[1, deep], preferred_element_type=F32)
        kept = product if kept is None else kept + product
    swap.wait_recv()
    out_ref[...] = kept + hrecv[...]
    swap.wait_send()

    def drain(ref, sem):
        pltpu.make_async_copy(ref, ref, sem).wait()

    @pl.when(resting)
    def _():
        drain(qsend, qs_send)
        drain(asend, as_send)

    @pl.when(owning)
    def _():
        drain(qsend.at[pl.ds(0, m - 1)], qs_send)
        drain(asend.at[:, pl.ds(0, m - 1)], as_send)
        drain(tally, qg_send)
        drain(tally, ag_send)


def solution(mesh):
    n = mesh.shape["seq"]
    m = max(n // 2, 2)

    def shards(hidden, gain, wq, keys, values, knew, vnew, lengths, wout):
        rows, depth = hidden.shape
        heads = wq.shape[1] // HD
        share = rows // m
        piece = share // 2
        block = keys.shape[1]
        half = wout.shape[1] // 2
        hc = heads // CHUNKS
        anywhere = pl.BlockSpec(memory_space=pl.ANY)
        dma = pltpu.SemaphoreType.DMA
        return pl.pallas_call(
            functools.partial(kernel, n, heads, rows, m, CUTS, CHUNKS),
            out_shape=pltpu.VMEM((rows, half), F32),
            in_specs=[anywhere] * 9,
            out_specs=pl.BlockSpec(memory_space=pltpu.VMEM),
            scratch_shapes=[
                pltpu.SMEM((rows,), jnp.int32),
                pltpu.VMEM((rows, depth), BF16),
                pltpu.VMEM((depth // HD, HD), BF16),
                pltpu.VMEM(wq.shape, BF16),
                pltpu.VMEM((rows // 2, block, HD), BF16),
                pltpu.VMEM((rows // 2, block, HD), BF16),
                pltpu.VMEM((2, rows, HD), BF16),
                pltpu.VMEM((2, wout.shape[0], half), BF16),
                pltpu.VMEM((2, rows, HD), F32),
                pltpu.VMEM((m, heads + 1, share, HD), F32),
                pltpu.VMEM((2 * n, heads + 1, share, HD), F32),
                pltpu.VMEM((2 * hc, share, HD), F32),
                pltpu.VMEM((CHUNKS, piece, 2 * hc, HD), F32),
                pltpu.VMEM((CHUNKS, m, piece, 2 * hc, HD), F32),
                pltpu.VMEM((CHUNKS, m, piece * 2 * hc + 8, HD), F32),
                pltpu.VMEM((CHUNKS, 2, n, piece * 2 * hc + 8, HD), F32),
                pltpu.VMEM((CHUNKS, 2, piece, hc, HD), F32),
                pltpu.VMEM((CHUNKS, rows, hc, HD), F32),
                pltpu.VMEM((rows, half), F32),
                pltpu.VMEM((rows, half), F32),
                pltpu.VMEM((CHUNKS, 2 * n - 1, piece, 2 * hc, HD), F32),
                dma((4,)),
                dma((CUTS,)),
                dma((2,)),
                dma(()),
                dma(()),
                dma((CHUNKS,)),
                dma(()),
                dma((CHUNKS, m)),
                dma(()),
                dma((CHUNKS, 2)),
                dma(()),
                dma((CHUNKS,)),
                dma((2,)),
            ],
            compiler_params=pltpu.CompilerParams(collective_id=0, has_side_effects=True),
            name="decode_step",
        )(lengths, hidden, gain.reshape(-1, HD), wq, keys, values, knew, vnew, wout)

    placed = (
        P(("groups", "batch"), "seq"),
        P("seq"),
        P("seq", "head"),
        P(("groups", "batch"), "seq", None),
        P(("groups", "batch"), "seq", None),
        P(("groups", "batch"), None),
        P(("groups", "batch"), None),
        P(("groups", "batch")),
        P("head", "seq"),
    )
    return jax.shard_map(
        shards,
        mesh=mesh,
        in_specs=placed,
        out_specs=P(("groups", "batch"), ("seq", "head")),
        check_vma=False,
    )
```

```python
import functools

import jax
import jax.numpy as jnp
from jax import lax
from jax.experimental import pallas as pl
from jax.experimental.pallas import tpu as pltpu
from jax.sharding import PartitionSpec as P

HD = 128
EPS = 1e-05
MESH = pl.DeviceIdType.MESH
F32 = jnp.float32
BF16 = jnp.bfloat16
EDGES = (0, 2, 4, 8, 16)
CHUNKS = 2


def outside_in(n):
    order = []
    for k in range((n + 1) // 2):
        order += [k] if k == n - 1 - k else [k, n - 1 - k]
    return order


def kernel(
    n,
    heads,
    rows,
    m,
    cuts,
    chunks,
    lens_hbm,
    hidden_hbm,
    gain_hbm,
    wq_hbm,
    keys_hbm,
    values_hbm,
    knew_hbm,
    vnew_hbm,
    wout_hbm,
    out_ref,
    lens_ref,
    hid,
    gain,
    wq,
    kbuf,
    vbuf,
    newb,
    wout,
    newf,
    qsend,
    qrecv,
    qturn,
    qown,
    qall,
    asend,
    arecv,
    aout,
    att,
    hsend,
    hrecv,
    tally,
    in_sem,
    wq_sem,
    kv_sem,
    wo_sem,
    qs_send,
    qs_recv,
    qg_send,
    qg_recv,
    as_send,
    as_recv,
    ag_send,
    ag_recv,
    h_sem,
):
    me = lax.axis_index("seq")
    core = lax.axis_index("head")
    other = 1 - core
    first = (n - m) // 2
    share = rows // m
    piece = share // 2
    half_rows = rows // 2
    block = keys_hbm.shape[1]
    width = wq_hbm.shape[0] * n
    hc = heads // chunks
    full = 2 * hc
    wide = full // 8 * piece
    on_chip = jnp.logical_and(me >= first, me < first + m)
    owning = jnp.logical_and(on_chip, core == 1)
    resting = jnp.logical_not(owning)
    my_j = jnp.clip(me - first, 0, m - 1)
    order = outside_in(n)

    def device(z, h):
        return {"seq": z, "head": h}

    def is_me(z, h):
        return jnp.logical_and(me == z, core == h)

    def not_me(z, h):
        return jnp.logical_not(is_me(z, h))

    barrier = pltpu.get_barrier_semaphore()

    def greet(z, h):
        pl.semaphore_signal(barrier, inc=1, device_id=device(z, h), device_id_type=MESH)

    for z in order:
        for h in (0, 1):
            meet = not_me(z, h)
            if h == 0 or not first <= z < first + m:
                partner = jnp.logical_and(me == z, core == 1 - h)
                meet = jnp.logical_and(meet, jnp.logical_or(owning, partner))
            pl.when(meet)(functools.partial(greet, z, h))
    greeted = jnp.where(owning, 2 * n - 1, jnp.where(on_chip, m, m + 1))

    ins = [
        pltpu.make_async_copy(src, dst, in_sem.at[i])
        for i, src, dst in (
            (0, hidden_hbm, hid),
            (1, gain_hbm, gain),
            (2, knew_hbm, newb.at[0]),
            (2, vnew_hbm, newb.at[1]),
            (3, lens_hbm, lens_ref),
        )
    ]
    for copy in ins[:2]:
        copy.start()
    wq_copies = []
    for c in range(len(cuts) - 1):
        cols = pl.ds(cuts[c] * HD, (cuts[c + 1] - cuts[c]) * HD)
        wq_copies.append(pltpu.make_async_copy(wq_hbm.at[:, cols], wq.at[:, cols], wq_sem.at[c]))
        wq_copies[-1].start()
    for copy in ins[2:]:
        copy.start()
    group = pl.ds(core * half_rows, half_rows)
    half = wout_hbm.shape[1] // 2
    later = [
        pltpu.make_async_copy(keys_hbm.at[group], kbuf, kv_sem.at[0]),
        pltpu.make_async_copy(values_hbm.at[group], vbuf, kv_sem.at[1]),
    ]
    for i, side in enumerate((other, core)):
        cols = pl.ds(pl.multiple_of(side * half, HD), half)
        later.append(pltpu.make_async_copy(wout_hbm.at[:, cols], wout.at[i], wo_sem))

    ins[0].wait()
    ins[1].wait()
    x = hid[...].astype(F32)
    x = jnp.concatenate(
        [
            x[u * half_rows + j * piece : u * half_rows + (j + 1) * piece]
            for j in range(m)
            for u in (0, 1)
        ],
        axis=0,
    )
    squares = jnp.sum(x * x, axis=-1, keepdims=True)
    g = gain[...].astype(F32)
    scaled = jnp.concatenate(
        [x[:, i * HD : (i + 1) * HD] * g[i : i + 1] for i in range(g.shape[0])], axis=1
    )
    upper = scaled.astype(BF16)
    lower = (scaled - upper.astype(F32)).astype(BF16)
    both = jnp.concatenate([upper, lower], axis=0)
    for j in range(m):
        qsend[j, 0] = jnp.broadcast_to(squares[j * share : (j + 1) * share], (share, HD))

    def span(c):
        start = cuts[c] + 1 if c else 0
        return pl.ds(start, cuts[c + 1] + 1 - start)

    def partial_send(c, j):
        return pltpu.make_async_remote_copy(
            src_ref=qsend.at[j, span(c)],
            dst_ref=qrecv.at[2 * me + core, span(c)],
            send_sem=qs_send,
            recv_sem=qs_recv.at[cuts[c] // hc],
            device_id=device(first + j, 1),
            device_id_type=MESH,
        )

    def place_own(j, c):
        qrecv[2 * me + 1, span(c)] = qsend[j, span(c)]

    for c in range(len(cuts) - 1):
        wq_copies[c].wait()
        if c == len(cuts) - 2:
            for copy in later:
                copy.start()
        product = jnp.dot(
            both, wq[:, cuts[c] * HD : cuts[c + 1] * HD], preferred_element_type=F32
        )
        part = product[:rows] + product[rows:]
        for h in range(cuts[c + 1] - cuts[c]):
            for j in range(m):
                qsend[j, cuts[c] + h + 1] = part[
                    j * share : (j + 1) * share, h * HD : (h + 1) * HD
                ]
        if c == 0:
            pl.semaphore_wait(barrier, greeted)
        for j in range(m):
            pl.when(not_me(first + j, 1))(partial_send(c, j).start)
            pl.when(is_me(first + j, 1))(functools.partial(place_own, j, c))

    pltpu.make_async_copy(newb, newb, in_sem.at[2]).wait()
    ins[4].wait()
    newf[...] = newb[...].astype(F32)

    def query_sends(c):
        return [
            (
                not_me(z, u),
                pltpu.make_async_remote_copy(
                    src_ref=qall.at[c, my_j] if u else qown.at[c],
                    dst_ref=qall.at[c, my_j],
                    send_sem=qg_send,
                    recv_sem=qg_recv.at[c, my_j],
                    device_id=device(z, u),
                    device_id_type=MESH,
                ),
            )
            for z in reversed(order)
            for u in (0, 1)
        ]

    @pl.when(owning)
    def _():
        for c in range(chunks):
            lo = 0 if c == 0 else 1 + c * hc
            arrived = qrecv.at[pl.ds(0, 2 * n - 1), pl.ds(lo, 1 + (c + 1) * hc - lo)]
            pltpu.make_async_copy(arrived, arrived, qs_recv.at[c]).wait()
            total = functools.reduce(jnp.add, [qrecv[2 * z + 1, 0] for z in range(n)])
            inv = lax.rsqrt(total / width + EPS) * (1.0 / HD**0.5)
            for h in (0, 1):
                planes = pl.ds(1 + c * hc, hc)
                q = functools.reduce(jnp.add, [qrecv[2 * z + h, planes] for z in range(n)])
                qturn[h * hc : (h + 1) * hc] = (q * inv[None]).astype(BF16).astype(F32)
            for r in range(piece):
                qown[c, r] = qturn[:, r, :]
                qall[c, my_j, r] = qturn[:, piece + r, :]
            for go, copy in query_sends(c):
                pl.when(go)(copy.start)

    lanes = lax.broadcasted_iota(jnp.int32, (full, HD), 1)
    lanes = lanes - lax.broadcasted_iota(jnp.int32, (full, HD), 0) // 8 * piece
    positions = me * block + lax.broadcasted_iota(jnp.int32, (full, block), 1)

    def keep_own(c):
        arecv[c, 1, me] = asend[c, my_j]

    def result_send(c, j):
        return pltpu.make_async_remote_copy(
            src_ref=asend.at[c, j],
            dst_ref=arecv.at[c, core, me],
            send_sem=as_send,
            recv_sem=as_recv.at[c, core],
            device_id=device(first + j, 1),
            device_id_type=MESH,
        )

    for c in range(chunks):
        for k in range(m):
            j = lax.rem(my_j + k, m)
            arrival = pltpu.make_async_remote_copy(
                src_ref=qall.at[c, j],
                dst_ref=qall.at[c, j],
                send_sem=qg_send,
                recv_sem=qg_recv.at[c, j],
                device_id=device(me, other),
                device_id_type=MESH,
            )
            pl.when(not_me(first + j, 1))(arrival.wait_recv)
            if c == 0 and k == 0:
                later[0].wait()
            scores, own = [], []
            for r in range(piece):
                q = qall[c, j, r]
                scores.append(
                    lax.dot_general(
                        q.astype(BF16),
                        kbuf[j * piece + r],
                        (((1,), (1,)), ((), ())),
                        preferred_element_type=F32,
                    )
                )
                row = core * half_rows + j * piece + r
                own.append(jnp.sum(q * newf[0, pl.ds(row, 1)], axis=-1, keepdims=True))
            if c == 0 and k == 0:
                later[1].wait()
            stats = jnp.zeros((full, HD), F32)
            for r in range(piece):
                live = positions < lens_ref[core * half_rows + j * piece + r]
                masked = jnp.where(live, scores[r], -jnp.inf)
                top = jnp.maximum(jnp.max(masked, axis=-1, keepdims=True), own[r])
                weights = jnp.exp(masked - top)
                weight = jnp.sum(weights, axis=-1, keepdims=True)
                for i, column in enumerate((top, weight, own[r])):
                    stats = jnp.where(lanes == i * wide + r, column, stats)
                asend[c, j, r * full : (r + 1) * full] = jnp.dot(
                    weights.astype(BF16), vbuf[j * piece + r], preferred_element_type=F32
                )
            asend[c, j, piece * full : piece * full + 8] = functools.reduce(
                jnp.add, [stats[i : i + 8] for i in range(0, full, 8)]
            )
            pl.when(not_me(first + j, 1))(result_send(c, j).start)
            pl.when(is_me(first + j, 1))(functools.partial(keep_own, c))

    def returns(c, u, stops):
        group = pl.ds(u * half_rows + my_j * piece, piece)
        return [
            (
                not_me(z, h),
                pltpu.make_async_remote_copy(
                    src_ref=att.at[c, group] if h else aout.at[c, u],
                    dst_ref=att.at[c, group],
                    send_sem=ag_send,
                    recv_sem=ag_recv.at[c],
                    device_id=device(z, h),
                    device_id_type=MESH,
                ),
            )
            for z in stops
            for h in (0, 1)
        ]

    @pl.when(owning)
    def _():
        for c in range(chunks):
            for u in (1, 0):
                arrived = arecv.at[c, u, pl.ds(0, n - u)]
                pltpu.make_async_copy(arrived, arrived, as_recv.at[c, u]).wait()
                stats = [arecv[c, u, z, piece * full : piece * full + 8] for z in range(n)]
                tops = [s[:, :wide] for s in stats]
                top = functools.reduce(jnp.maximum, tops)
                fresh = jnp.exp(stats[0][:, 2 * wide : 3 * wide] - top)
                factors = [jnp.exp(t - top) for t in tops]
                totals = fresh
                for z in range(n):
                    totals = totals + stats[z][:, wide : 2 * wide] * factors[z]
                inverse = 1.0 / totals
                fresh = fresh * inverse
                factors = [f * inverse for f in factors]
                for r in range(piece):
                    row = u * half_rows + my_j * piece + r
                    for t in range(full // 8):
                        at = t * piece + r
                        result = fresh[:, at : at + 1] * newf[1, pl.ds(row, 1)]
                        for z in range(n):
                            part = arecv[c, u, z, r * full + t * 8 : r * full + t * 8 + 8]
                            result = result + part * factors[z][:, at : at + 1]
                        result = result.astype(BF16).astype(F32)
                        if t * 8 < hc:
                            aout[c, u, r, t * 8 : t * 8 + 8] = result
                        else:
                            att[c, row, t * 8 - hc : t * 8 - hc + 8] = result
                if c < chunks - 1:
                    ready = returns(c, u, order)
                else:
                    ready = returns(c, u, order[:2])
                    if u == 0:
                        ready += returns(c, 1, order[2:]) + returns(c, 0, order[2:])
                for go, copy in ready:
                    pl.when(go)(copy.start)

    sent, kept = None, None
    for c in range(chunks):
        for owner, count in ((owning, rows - share), (resting, rows)):
            arrived = att.at[c, pl.ds(0, count)]
            pl.when(owner)(pltpu.make_async_copy(arrived, arrived, ag_recv.at[c]).wait)
        if c == 0:
            pltpu.make_async_copy(wout, wout, wo_sem).wait()
        attended = jnp.concatenate([att[c, :, h, :] for h in range(hc)], axis=1).astype(BF16)
        deep = slice(c * hc * HD, (c + 1) * hc * HD)
        product = jnp.dot(attended, wout[0, deep], preferred_element_type=F32)
        sent = product if sent is None else sent + product
        if c == chunks - 1:
            hsend[...] = sent
            swap = pltpu.make_async_remote_copy(
                src_ref=hsend,
                dst_ref=hrecv,
                send_sem=h_sem.at[0],
                recv_sem=h_sem.at[1],
                device_id=device(me, other),
                device_id_type=MESH,
            )
            swap.start()
        product = jnp.dot(attended, wout[1, deep], preferred_element_type=F32)
        kept = product if kept is None else kept + product
    swap.wait_recv()
    out_ref[...] = kept + hrecv[...]
    swap.wait_send()

    def drain(ref, sem):
        pltpu.make_async_copy(ref, ref, sem).wait()

    @pl.when(resting)
    def _():
        drain(qsend, qs_send)
        drain(asend, as_send)

    @pl.when(owning)
    def _():
        drain(qsend.at[pl.ds(0, m - 1)], qs_send)
        drain(asend.at[:, pl.ds(0, m - 1)], as_send)
        drain(tally, qg_send)
        drain(tally, ag_send)


def solution(mesh):
    n = mesh.shape["seq"]
    m = max(n // 2, 2)

    def shards(hidden, gain, wq, keys, values, knew, vnew, lengths, wout):
        rows, depth = hidden.shape
        heads = wq.shape[1] // HD
        share = rows // m
        piece = share // 2
        block = keys.shape[1]
        half = wout.shape[1] // 2
        hc = heads // CHUNKS
        cuts = tuple(heads * e // EDGES[-1] for e in EDGES)
        anywhere = pl.BlockSpec(memory_space=pl.ANY)
        dma = pltpu.SemaphoreType.DMA
        return pl.pallas_call(
            functools.partial(kernel, n, heads, rows, m, cuts, CHUNKS),
            out_shape=pltpu.VMEM((rows, half), F32),
            in_specs=[anywhere] * 9,
            out_specs=pl.BlockSpec(memory_space=pltpu.VMEM),
            scratch_shapes=[
                pltpu.SMEM((rows,), jnp.int32),
                pltpu.VMEM((rows, depth), BF16),
                pltpu.VMEM((depth // HD, HD), BF16),
                pltpu.VMEM(wq.shape, BF16),
                pltpu.VMEM((rows // 2, block, HD), BF16),
                pltpu.VMEM((rows // 2, block, HD), BF16),
                pltpu.VMEM((2, rows, HD), BF16),
                pltpu.VMEM((2, wout.shape[0], half), BF16),
                pltpu.VMEM((2, rows, HD), F32),
                pltpu.VMEM((m, heads + 1, share, HD), F32),
                pltpu.VMEM((2 * n, heads + 1, share, HD), F32),
                pltpu.VMEM((2 * hc, share, HD), F32),
                pltpu.VMEM((CHUNKS, piece, 2 * hc, HD), F32),
                pltpu.VMEM((CHUNKS, m, piece, 2 * hc, HD), F32),
                pltpu.VMEM((CHUNKS, m, piece * 2 * hc + 8, HD), F32),
                pltpu.VMEM((CHUNKS, 2, n, piece * 2 * hc + 8, HD), F32),
                pltpu.VMEM((CHUNKS, 2, piece, hc, HD), F32),
                pltpu.VMEM((CHUNKS, rows, hc, HD), F32),
                pltpu.VMEM((rows, half), F32),
                pltpu.VMEM((rows, half), F32),
                pltpu.VMEM((CHUNKS, 2 * n - 1, piece, 2 * hc, HD), F32),
                dma((4,)),
                dma((len(cuts) - 1,)),
                dma((2,)),
                dma(()),
                dma(()),
                dma((CHUNKS,)),
                dma(()),
                dma((CHUNKS, m)),
                dma(()),
                dma((CHUNKS, 2)),
                dma(()),
                dma((CHUNKS,)),
                dma((2,)),
            ],
            compiler_params=pltpu.CompilerParams(collective_id=0, has_side_effects=True),
            name="decode_step",
        )(lengths, hidden, gain.reshape(-1, HD), wq, keys, values, knew, vnew, wout)

    placed = (
        P(("groups", "batch"), "seq"),
        P("seq"),
        P("seq", "head"),
        P(("groups", "batch"), "seq", None),
        P(("groups", "batch"), "seq", None),
        P(("groups", "batch"), None),
        P(("groups", "batch"), None),
        P(("groups", "batch")),
        P("head", "seq"),
    )
    return jax.shard_map(
        shards,
        mesh=mesh,
        in_specs=placed,
        out_specs=P(("groups", "batch"), ("seq", "head")),
        check_vma=False,
    )
```

```python
import functools

import jax
import jax.numpy as jnp
from jax import lax
from jax.experimental import pallas as pl
from jax.experimental.pallas import tpu as pltpu
from jax.sharding import PartitionSpec as P

HD = 128
EPS = 1e-05
MESH = pl.DeviceIdType.MESH
F32 = jnp.float32
BF16 = jnp.bfloat16
EDGES = (0, 2, 4, 8, 16)
CHUNKS = 2
UNITS = (0, 4, 8, 16)


def outside_in(n):
    order = []
    for k in range((n + 1) // 2):
        order += [k] if k == n - 1 - k else [k, n - 1 - k]
    return order


def kernel(
    n,
    heads,
    rows,
    m,
    cuts,
    chunks,
    units,
    lens_hbm,
    hidden_hbm,
    gain_hbm,
    wq_hbm,
    keys_hbm,
    values_hbm,
    knew_hbm,
    vnew_hbm,
    wout_hbm,
    out_ref,
    lens_ref,
    hid,
    gain,
    wq,
    kbuf,
    vbuf,
    newb,
    wout,
    newf,
    qsend,
    qrecv,
    qturn,
    qown,
    qall,
    kturn,
    ssend,
    srecv,
    coef,
    asend,
    arecv,
    aout,
    att,
    hsend,
    hrecv,
    tally,
    in_sem,
    wq_sem,
    kv_sem,
    wo_sem,
    qs_send,
    qs_recv,
    qg_send,
    qg_recv,
    ss_send,
    ss_recv,
    as_send,
    as_recv,
    ag_send,
    ag_recv,
    h_sem,
):
    me = lax.axis_index("seq")
    core = lax.axis_index("head")
    other = 1 - core
    first = (n - m) // 2
    share = rows // m
    piece = share // 2
    half_rows = rows // 2
    block = keys_hbm.shape[1]
    width = wq_hbm.shape[0] * n
    hc = heads // chunks
    full = 2 * hc
    subs = 1
    part_rows = piece
    squared = units[1]
    each = 2 * part_rows
    on_chip = jnp.logical_and(me >= first, me < first + m)
    owning = jnp.logical_and(on_chip, core == 1)
    resting = jnp.logical_not(owning)
    my_j = jnp.clip(me - first, 0, m - 1)
    order = outside_in(n)

    def device(z, h):
        return {"seq": z, "head": h}

    def is_me(z, h):
        return jnp.logical_and(me == z, core == h)

    def not_me(z, h):
        return jnp.logical_not(is_me(z, h))

    barrier = pltpu.get_barrier_semaphore()

    def greet(z, h):
        pl.semaphore_signal(barrier, inc=1, device_id=device(z, h), device_id_type=MESH)

    for z in order:
        for h in (0, 1):
            meet = not_me(z, h)
            if h == 0 or not first <= z < first + m:
                partner = jnp.logical_and(me == z, core == 1 - h)
                meet = jnp.logical_and(meet, jnp.logical_or(owning, partner))
            pl.when(meet)(functools.partial(greet, z, h))
    greeted = jnp.where(owning, 2 * n - 1, jnp.where(on_chip, m, m + 1))

    ins = [
        pltpu.make_async_copy(src, dst, in_sem.at[i])
        for i, src, dst in (
            (0, hidden_hbm, hid),
            (1, gain_hbm, gain),
            (2, knew_hbm, newb.at[0]),
            (2, vnew_hbm, newb.at[1]),
            (3, lens_hbm, lens_ref),
        )
    ]
    for copy in ins[:2]:
        copy.start()
    wq_copies = []
    for c in range(len(cuts) - 1):
        cols = pl.ds(cuts[c] * HD, (cuts[c + 1] - cuts[c]) * HD)
        wq_copies.append(pltpu.make_async_copy(wq_hbm.at[:, cols], wq.at[:, cols], wq_sem.at[c]))
        wq_copies[-1].start()
    for copy in ins[2:]:
        copy.start()
    group = pl.ds(core * half_rows, half_rows)
    half = wout_hbm.shape[1] // 2
    later = [
        pltpu.make_async_copy(keys_hbm.at[group], kbuf, kv_sem.at[0]),
        pltpu.make_async_copy(values_hbm.at[group], vbuf, kv_sem.at[1]),
    ]
    for i, side in enumerate((other, core)):
        cols = pl.ds(pl.multiple_of(side * half, HD), half)
        later.append(pltpu.make_async_copy(wout_hbm.at[:, cols], wout.at[i], wo_sem))

    ins[0].wait()
    ins[1].wait()
    x = hid[...].astype(F32)
    x = jnp.concatenate(
        [
            x[u * half_rows + j * piece : u * half_rows + (j + 1) * piece]
            for j in range(m)
            for u in (0, 1)
        ],
        axis=0,
    )
    g = gain[...].astype(F32)
    scaled = jnp.concatenate(
        [x[:, i * HD : (i + 1) * HD] * g[i : i + 1] for i in range(g.shape[0])], axis=1
    )
    upper = scaled.astype(BF16)
    lower = (scaled - upper.astype(F32)).astype(BF16)
    both = jnp.concatenate([upper, lower], axis=0)
    def place_squares():
        squares = jnp.sum(x * x, axis=-1, keepdims=True)
        for j in range(m):
            qsend[j, squared] = jnp.broadcast_to(squares[j * share : (j + 1) * share], (share, HD))


    def unit_of(head):
        return sum(edge <= head for edge in units) - 1

    def span(c):
        start = cuts[c] + (cuts[c] >= squared)
        return pl.ds(start, cuts[c + 1] + (cuts[c + 1] >= squared) - start)

    def partial_send(c, j):
        return pltpu.make_async_remote_copy(
            src_ref=qsend.at[j, span(c)],
            dst_ref=qrecv.at[2 * me + core, span(c)],
            send_sem=qs_send,
            recv_sem=qs_recv.at[unit_of(cuts[c])],
            device_id=device(first + j, 1),
            device_id_type=MESH,
        )

    def place_own(j, c):
        qrecv[2 * me + 1, span(c)] = qsend[j, span(c)]

    for c in range(len(cuts) - 1):
        wq_copies[c].wait()
        if c == len(cuts) - 2:
            for copy in later:
                copy.start()
        product = jnp.dot(
            both, wq[:, cuts[c] * HD : cuts[c + 1] * HD], preferred_element_type=F32
        )
        part = product[:rows] + product[rows:]
        for h in range(cuts[c + 1] - cuts[c]):
            for j in range(m):
                qsend[j, cuts[c] + (cuts[c] >= squared) + h] = part[
                    j * share : (j + 1) * share, h * HD : (h + 1) * HD
                ]
        if cuts[c + 1] == squared:
            place_squares()
        if c == 0:
            pl.semaphore_wait(barrier, greeted)
        for j in range(m):
            pl.when(not_me(first + j, 1))(partial_send(c, j).start)
            pl.when(is_me(first + j, 1))(functools.partial(place_own, j, c))

    pltpu.make_async_copy(newb, newb, in_sem.at[2]).wait()
    ins[4].wait()
    newf[...] = newb[...].astype(F32)

    def flip(k):
        j = lax.rem(my_j + k, m)
        for r in range(piece):
            kturn[j * piece + r] = kbuf[j * piece + r].T

    later[0].wait()
    flip(0)

    @pl.when(resting)
    def _():
        for k in range(1, m):
            flip(k)

    lanes = lax.broadcasted_iota(jnp.int32, (full, HD), 1)
    lanes = lanes - lax.broadcasted_iota(jnp.int32, (full, HD), 0) * each

    tiles = [
        (units[i] // hc, pl.ds(units[i] % hc * 2, (units[i + 1] - units[i]) * 2))
        for i in range(len(units) - 1)
    ]

    def query_sends(i):
        c, part = tiles[i]
        return [
            (
                not_me(z, u),
                pltpu.make_async_remote_copy(
                    src_ref=(qall.at[c, my_j] if u else qown.at[c]).at[:, part],
                    dst_ref=qall.at[c, my_j].at[:, part],
                    send_sem=qg_send,
                    recv_sem=qg_recv.at[i, my_j],
                    device_id=device(z, u),
                    device_id_type=MESH,
                ),
            )
            for u in (0, 1)
            for z in order
        ]

    @pl.when(owning)
    def _():
        for i in range(len(units) - 1):
            c, part = tiles[i]
            size = units[i + 1] - units[i]
            lo = units[i] + (i > 0)
            arrived = qrecv.at[pl.ds(0, 2 * n - 1), pl.ds(lo, size + (i == 0))]
            pltpu.make_async_copy(arrived, arrived, qs_recv.at[i]).wait()
            total = functools.reduce(jnp.add, [qrecv[2 * z + 1, squared] for z in range(n)])
            inv = lax.rsqrt(total / width + EPS) * (1.0 / HD**0.5)
            for t in range(size // 4):
                for h in (0, 1):
                    planes = pl.ds(lo + t * 4, 4)
                    q = functools.reduce(jnp.add, [qrecv[2 * z + h, planes] for z in range(n)])
                    q = (q * inv[None]).astype(BF16).astype(F32)
                    qturn[t * 8 + h * 4 : t * 8 + h * 4 + 4] = q
            for r in range(piece):
                qown[c, r, part] = qturn[: 2 * size, r, :]
                qall[c, my_j, r, part] = qturn[: 2 * size, piece + r, :]
            for go, copy in query_sends(i):
                pl.when(go)(copy.start)
            if units[i + 1] == hc:
                for k in range(1, m):
                    flip(k)

    lanes = lax.broadcasted_iota(jnp.int32, (full, HD), 1)
    lanes = lanes - lax.broadcasted_iota(jnp.int32, (full, HD), 0) * each
    positions = me * block + lax.broadcasted_iota(jnp.int32, (full, block), 1)

    def keep_own(c):
        for s in range(subs):
            arecv[c, s, 1, me] = asend[c, my_j, s]
            srecv[c, s, n + me] = ssend[c, my_j, s]

    def stats_send(c, j, s):
        return pltpu.make_async_remote_copy(
            src_ref=ssend.at[c, j, s],
            dst_ref=srecv.at[c, s, core * n + me],
            send_sem=ss_send,
            recv_sem=ss_recv.at[c, s],
            device_id=device(first + j, 1),
            device_id_type=MESH,
        )

    def result_send(c, j, s):
        return pltpu.make_async_remote_copy(
            src_ref=asend.at[c, j, s],
            dst_ref=arecv.at[c, s, core, me],
            send_sem=as_send,
            recv_sem=as_recv.at[c, s, core],
            device_id=device(first + j, 1),
            device_id_type=MESH,
        )

    adds = jnp.where(me == n // 2, 1.0, 0.0)

    for c in range(chunks):
        for k in range(m):
            j = lax.rem(my_j + m - 1 - k, m)
            for i, (chunk, part) in enumerate(tiles):
                if chunk == c:
                    arrival = pltpu.make_async_remote_copy(
                        src_ref=qall.at[c, j].at[:, part],
                        dst_ref=qall.at[c, j].at[:, part],
                        send_sem=qg_send,
                        recv_sem=qg_recv.at[i, j],
                        device_id=device(me, other),
                        device_id_type=MESH,
                    )
                    pl.when(not_me(first + j, 1))(arrival.wait_recv)
            scores, own = [], []
            for r in range(piece):
                q = qall[c, j, r]
                scores.append(
                    jnp.dot(q.astype(BF16), kturn[j * piece + r], preferred_element_type=F32)
                )
                row = core * half_rows + j * piece + r
                own.append(jnp.sum(q * newf[0, pl.ds(row, 1)], axis=-1, keepdims=True))
            if c == 0 and k == 0:
                later[1].wait()
            for s in range(subs):
                stats = jnp.zeros((full, HD), F32)
                for i in range(part_rows):
                    r = s * part_rows + i
                    row = core * half_rows + j * piece + r
                    live = positions < lens_ref[row]
                    masked = jnp.where(live, scores[r], -jnp.inf)
                    top = jnp.maximum(jnp.max(masked, axis=-1, keepdims=True), own[r])
                    weights = jnp.exp(masked - top)
                    fresh = jnp.exp(own[r] - top) * adds
                    weight = jnp.sum(weights, axis=-1, keepdims=True) + fresh
                    stats = jnp.where(lanes == 2 * i, top, stats)
                    stats = jnp.where(lanes == 2 * i + 1, weight, stats)
                    product = jnp.dot(
                        weights.astype(BF16), vbuf[j * piece + r], preferred_element_type=F32
                    )
                    product = product + fresh * newf[1, pl.ds(row, 1)]
                    asend[c, j, s, i * full : (i + 1) * full] = product
                ssend[c, j, s] = jnp.sum(stats, axis=0, keepdims=True)

            @pl.when(not_me(first + j, 1))
            def _(c=c, j=j):
                for s in range(subs):
                    stats_send(c, j, s).start()
                    result_send(c, j, s).start()

            pl.when(is_me(first + j, 1))(functools.partial(keep_own, c))

    def returns(c, s, u, stops):
        group = pl.ds(u * half_rows + my_j * piece + s * part_rows, part_rows)
        return [
            (
                not_me(z, h),
                pltpu.make_async_remote_copy(
                    src_ref=att.at[c, group] if h else aout.at[c, s, u],
                    dst_ref=att.at[c, group],
                    send_sem=ag_send,
                    recv_sem=ag_recv.at[c],
                    device_id=device(z, h),
                    device_id_type=MESH,
                ),
            )
            for z in stops
            for h in (0, 1)
        ]

    def share_out(c, s):
        arrived = srecv.at[c, s, pl.ds(0, 2 * n - 1)]
        pltpu.make_async_copy(arrived, arrived, ss_recv.at[c, s]).wait()
        for u in (1, 0):
            stats = [jnp.broadcast_to(srecv[c, s, u * n + z], (8, HD)) for z in range(n)]
            top = functools.reduce(jnp.maximum, stats)
            factors = [jnp.exp(line - top) for line in stats]
            totals = functools.reduce(
                jnp.add, [pltpu.roll(stats[z], HD - 1, 1) * factors[z] for z in range(n)]
            )
            inverse = 1.0 / totals
            for i in range(part_rows):
                for t in range(full // 8):
                    here = lanes[t * 8 : t * 8 + 8] == 2 * i
                    at = i * full + t * 8
                    for z, factor in enumerate(factors):
                        one = jnp.where(here, factor * inverse, 0.0)
                        one = jnp.sum(one, axis=-1, keepdims=True)
                        coef[u, z, at : at + 8] = jnp.broadcast_to(one, (8, HD))

    @pl.when(owning)
    def _():
        for c in range(chunks):
            for s in range(subs):
                last = c == chunks - 1 and s == subs - 1
                share_out(c, s)
                for u in (1, 0):
                    arrived = arecv.at[c, s, u, pl.ds(0, n - u)]
                    pltpu.make_async_copy(arrived, arrived, as_recv.at[c, s, u]).wait()
                    for i in range(part_rows):
                        row = u * half_rows + my_j * piece + s * part_rows + i
                        for t in range(full // 8):
                            at = slice(i * full + t * 8, i * full + t * 8 + 8)
                            result = functools.reduce(
                                jnp.add,
                                [coef[u, z, at] * arecv[c, s, u, z, at] for z in range(n)],
                            )
                            result = result.astype(BF16).astype(F32)
                            aout[c, s, u, i, t * 4 : t * 4 + 4] = result[:4]
                            att[c, row, t * 4 : t * 4 + 4] = result[4:]
                    if not last:
                        ready = returns(c, s, u, order)
                    else:
                        ready = returns(c, s, u, order[:2])
                        if u == 0:
                            ready += returns(c, s, 1, order[2:]) + returns(c, s, 0, order[2:])
                    for go, copy in ready:
                        pl.when(go)(copy.start)

    sent, kept = None, None
    for c in range(chunks):
        for owner, count in ((owning, rows - share), (resting, rows)):
            arrived = att.at[c, pl.ds(0, count)]
            pl.when(owner)(pltpu.make_async_copy(arrived, arrived, ag_recv.at[c]).wait)
        if c == 0:
            pltpu.make_async_copy(wout, wout, wo_sem).wait()
        attended = jnp.concatenate([att[c, :, h, :] for h in range(hc)], axis=1).astype(BF16)
        deep = slice(c * hc * HD, (c + 1) * hc * HD)
        product = jnp.dot(attended, wout[0, deep], preferred_element_type=F32)
        sent = product if sent is None else sent + product
        if c == chunks - 1:
            hsend[...] = sent
            swap = pltpu.make_async_remote_copy(
                src_ref=hsend,
                dst_ref=hrecv,
                send_sem=h_sem.at[0],
                recv_sem=h_sem.at[1],
                device_id=device(me, other),
                device_id_type=MESH,
            )
            swap.start()
        product = jnp.dot(attended, wout[1, deep], preferred_element_type=F32)
        kept = product if kept is None else kept + product
    swap.wait_recv()
    out_ref[...] = kept + hrecv[...]
    swap.wait_send()

    def drain(ref, sem):
        pltpu.make_async_copy(ref, ref, sem).wait()

    @pl.when(resting)
    def _():
        drain(qsend, qs_send)
        drain(asend, as_send)
        drain(ssend, ss_send)

    @pl.when(owning)
    def _():
        drain(qsend.at[pl.ds(0, m - 1)], qs_send)
        drain(asend.at[:, pl.ds(0, m - 1)], as_send)
        drain(ssend.at[:, pl.ds(0, m - 1)], ss_send)
        drain(tally, qg_send)
        drain(tally, ag_send)


def solution(mesh):
    n = mesh.shape["seq"]
    m = max(n // 2, 2)

    def shards(hidden, gain, wq, keys, values, knew, vnew, lengths, wout):
        rows, depth = hidden.shape
        heads = wq.shape[1] // HD
        share = rows // m
        piece = share // 2
        subs = 1
        units = tuple(heads * e // UNITS[-1] for e in UNITS)
        block = keys.shape[1]
        half = wout.shape[1] // 2
        hc = heads // CHUNKS
        cuts = tuple(heads * e // EDGES[-1] for e in EDGES)
        anywhere = pl.BlockSpec(memory_space=pl.ANY)
        dma = pltpu.SemaphoreType.DMA
        return pl.pallas_call(
            functools.partial(kernel, n, heads, rows, m, cuts, CHUNKS, units),
            out_shape=pltpu.VMEM((rows, half), F32),
            in_specs=[anywhere] * 9,
            out_specs=pl.BlockSpec(memory_space=pltpu.VMEM),
            scratch_shapes=[
                pltpu.SMEM((rows,), jnp.int32),
                pltpu.VMEM((rows, depth), BF16),
                pltpu.VMEM((depth // HD, HD), BF16),
                pltpu.VMEM(wq.shape, BF16),
                pltpu.VMEM((rows // 2, block, HD), BF16),
                pltpu.VMEM((rows // 2, block, HD), BF16),
                pltpu.VMEM((2, rows, HD), BF16),
                pltpu.VMEM((2, wout.shape[0], half), BF16),
                pltpu.VMEM((2, rows, HD), F32),
                pltpu.VMEM((m, heads + 1, share, HD), F32),
                pltpu.VMEM((2 * n, heads + 1, share, HD), F32),
                pltpu.VMEM((2 * hc, share, HD), F32),
                pltpu.VMEM((CHUNKS, piece, 2 * hc, HD), F32),
                pltpu.VMEM((CHUNKS, m, piece, 2 * hc, HD), F32),
                pltpu.VMEM((rows // 2, HD, block), BF16),
                pltpu.VMEM((CHUNKS, m, subs, 1, HD), F32),
                pltpu.VMEM((CHUNKS, subs, 2 * n, 1, HD), F32),
                pltpu.VMEM((2, n, piece // subs * 2 * hc, HD), F32),
                pltpu.VMEM((CHUNKS, m, subs, piece // subs * 2 * hc, HD), F32),
                pltpu.VMEM((CHUNKS, subs, 2, n, piece // subs * 2 * hc, HD), F32),
                pltpu.VMEM((CHUNKS, subs, 2, piece // subs, hc, HD), F32),
                pltpu.VMEM((CHUNKS, rows, hc, HD), F32),
                pltpu.VMEM((rows, half), F32),
                pltpu.VMEM((rows, half), F32),
                pltpu.VMEM((CHUNKS, 2 * n - 1, piece, 2 * hc, HD), F32),
                dma((4,)),
                dma((len(cuts) - 1,)),
                dma((2,)),
                dma(()),
                dma(()),
                dma((len(units) - 1,)),
                dma(()),
                dma((len(units) - 1, m)),
                dma(()),
                dma((CHUNKS, subs)),
                dma(()),
                dma((CHUNKS, subs, 2)),
                dma(()),
                dma((CHUNKS,)),
                dma((2,)),
            ],
            compiler_params=pltpu.CompilerParams(collective_id=0, has_side_effects=True),
            name="decode_step",
        )(lengths, hidden, gain.reshape(-1, HD), wq, keys, values, knew, vnew, wout)

    placed = (
        P(("groups", "batch"), "seq"),
        P("seq"),
        P("seq", "head"),
        P(("groups", "batch"), "seq", None),
        P(("groups", "batch"), "seq", None),
        P(("groups", "batch"), None),
        P(("groups", "batch"), None),
        P(("groups", "batch")),
        P("head", "seq"),
    )
    return jax.shard_map(
        shards,
        mesh=mesh,
        in_specs=placed,
        out_specs=P(("groups", "batch"), ("seq", "head")),
        check_vma=False,
    )
```

```python
import functools

import jax
import jax.numpy as jnp
from jax import lax
from jax.experimental import pallas as pl
from jax.experimental.pallas import tpu as pltpu
from jax.sharding import PartitionSpec as P

HD = 128
EPS = 1e-05
MESH = pl.DeviceIdType.MESH
F32 = jnp.float32
BF16 = jnp.bfloat16
EDGES = (0, 2, 4, 8, 16)
CHUNKS = 2
UNITS = (0, 2, 4, 8, 16)


def outside_in(n):
    order = []
    for k in range((n + 1) // 2):
        order += [k] if k == n - 1 - k else [k, n - 1 - k]
    return order


def kernel(
    n,
    heads,
    rows,
    m,
    cuts,
    chunks,
    units,
    lens_hbm,
    hidden_hbm,
    gain_hbm,
    wq_hbm,
    keys_hbm,
    values_hbm,
    knew_hbm,
    vnew_hbm,
    wout_hbm,
    out_ref,
    lens_ref,
    hid,
    gain,
    wq,
    kbuf,
    vbuf,
    newb,
    wout,
    newf,
    qsend,
    qrecv,
    qturn,
    qown,
    qall,
    kturn,
    ssend,
    srecv,
    coef,
    asend,
    arecv,
    aout,
    att,
    hsend,
    hrecv,
    tally,
    in_sem,
    wq_sem,
    kv_sem,
    wo_sem,
    qs_send,
    qs_recv,
    qg_send,
    qg_recv,
    ss_send,
    ss_recv,
    as_send,
    as_recv,
    ag_send,
    ag_recv,
    h_sem,
):
    me = lax.axis_index("seq")
    core = lax.axis_index("head")
    other = 1 - core
    first = (n - m) // 2
    share = rows // m
    piece = share // 2
    half_rows = rows // 2
    block = keys_hbm.shape[1]
    width = wq_hbm.shape[0] * n
    hc = heads // chunks
    full = 2 * hc
    subs = 1
    part_rows = piece
    squared = units[1]
    each = 2 * part_rows
    on_chip = jnp.logical_and(me >= first, me < first + m)
    owning = jnp.logical_and(on_chip, core == 1)
    resting = jnp.logical_not(owning)
    my_j = jnp.clip(me - first, 0, m - 1)
    order = outside_in(n)

    def device(z, h):
        return {"seq": z, "head": h}

    def is_me(z, h):
        return jnp.logical_and(me == z, core == h)

    def not_me(z, h):
        return jnp.logical_not(is_me(z, h))

    barrier = pltpu.get_barrier_semaphore()

    def greet(z, h):
        pl.semaphore_signal(barrier, inc=1, device_id=device(z, h), device_id_type=MESH)

    for z in order:
        for h in (0, 1):
            meet = not_me(z, h)
            if h == 0 or not first <= z < first + m:
                partner = jnp.logical_and(me == z, core == 1 - h)
                meet = jnp.logical_and(meet, jnp.logical_or(owning, partner))
            pl.when(meet)(functools.partial(greet, z, h))
    greeted = jnp.where(owning, 2 * n - 1, jnp.where(on_chip, m, m + 1))

    ins = [
        pltpu.make_async_copy(src, dst, in_sem.at[i])
        for i, src, dst in (
            (0, hidden_hbm, hid),
            (1, gain_hbm, gain),
            (2, knew_hbm, newb.at[0]),
            (2, vnew_hbm, newb.at[1]),
            (3, lens_hbm, lens_ref),
        )
    ]
    for copy in ins[:2]:
        copy.start()
    wq_copies = []
    for c in range(len(cuts) - 1):
        cols = pl.ds(cuts[c] * HD, (cuts[c + 1] - cuts[c]) * HD)
        wq_copies.append(pltpu.make_async_copy(wq_hbm.at[:, cols], wq.at[:, cols], wq_sem.at[c]))
        wq_copies[-1].start()
    for copy in ins[2:]:
        copy.start()
    group = pl.ds(core * half_rows, half_rows)
    half = wout_hbm.shape[1] // 2
    later = [
        pltpu.make_async_copy(keys_hbm.at[group], kbuf, kv_sem.at[0]),
        pltpu.make_async_copy(values_hbm.at[group], vbuf, kv_sem.at[1]),
    ]
    for i, side in enumerate((other, core)):
        cols = pl.ds(pl.multiple_of(side * half, HD), half)
        later.append(pltpu.make_async_copy(wout_hbm.at[:, cols], wout.at[i], wo_sem))

    ins[0].wait()
    ins[1].wait()
    x = hid[...].astype(F32)
    x = jnp.concatenate(
        [
            x[u * half_rows + j * piece : u * half_rows + (j + 1) * piece]
            for j in range(m)
            for u in (0, 1)
        ],
        axis=0,
    )
    g = gain[...].astype(F32)
    scaled = jnp.concatenate(
        [x[:, i * HD : (i + 1) * HD] * g[i : i + 1] for i in range(g.shape[0])], axis=1
    )
    upper = scaled.astype(BF16)
    lower = (scaled - upper.astype(F32)).astype(BF16)
    both = jnp.concatenate([upper, lower], axis=0)
    def place_squares():
        squares = jnp.sum(x * x, axis=-1, keepdims=True)
        for j in range(m):
            qsend[j, squared] = jnp.broadcast_to(squares[j * share : (j + 1) * share], (share, HD))


    def unit_of(head):
        return sum(edge <= head for edge in units) - 1

    def span(c):
        start = cuts[c] + (cuts[c] >= squared)
        return pl.ds(start, cuts[c + 1] + (cuts[c + 1] >= squared) - start)

    def partial_send(c, j):
        return pltpu.make_async_remote_copy(
            src_ref=qsend.at[j, span(c)],
            dst_ref=qrecv.at[2 * me + core, span(c)],
            send_sem=qs_send,
            recv_sem=qs_recv.at[unit_of(cuts[c])],
            device_id=device(first + j, 1),
            device_id_type=MESH,
        )

    def place_own(j, c):
        qrecv[2 * me + 1, span(c)] = qsend[j, span(c)]

    for c in range(len(cuts) - 1):
        wq_copies[c].wait()
        if c == len(cuts) - 2:
            for copy in later:
                copy.start()
        product = jnp.dot(
            both, wq[:, cuts[c] * HD : cuts[c + 1] * HD], preferred_element_type=F32
        )
        part = product[:rows] + product[rows:]
        for h in range(cuts[c + 1] - cuts[c]):
            for j in range(m):
                qsend[j, cuts[c] + (cuts[c] >= squared) + h] = part[
                    j * share : (j + 1) * share, h * HD : (h + 1) * HD
                ]
        if cuts[c + 1] == squared:
            place_squares()
        if c == 0:
            pl.semaphore_wait(barrier, greeted)
        for j in range(m):
            pl.when(not_me(first + j, 1))(partial_send(c, j).start)
            pl.when(is_me(first + j, 1))(functools.partial(place_own, j, c))

    pltpu.make_async_copy(newb, newb, in_sem.at[2]).wait()
    ins[4].wait()
    newf[...] = newb[...].astype(F32)

    def flip(k):
        j = lax.rem(my_j + k, m)
        for r in range(piece):
            kturn[j * piece + r] = kbuf[j * piece + r].T

    later[0].wait()
    flip(0)

    @pl.when(resting)
    def _():
        for k in range(1, m):
            flip(k)

    lanes = lax.broadcasted_iota(jnp.int32, (full, HD), 1)
    lanes = lanes - lax.broadcasted_iota(jnp.int32, (full, HD), 0) * each

    tiles = [
        (units[i] // hc, pl.ds(units[i] % hc * 2, (units[i + 1] - units[i]) * 2))
        for i in range(len(units) - 1)
    ]

    def runs_of(c):
        heads_at = []
        for lo, hi in zip(units[:-1], units[1:]):
            if lo // hc == c:
                heads_at += [(h, head % hc) for h in (0, 1) for head in range(lo, hi)]
        found = []
        for t in range(full // 8):
            found.append([])
            for at, (h, head) in enumerate(heads_at[t * 8 : t * 8 + 8]):
                if at and found[t][-1][1] == h and found[t][-1][2] + found[t][-1][3] == head:
                    found[t][-1][3] += 1
                else:
                    found[t].append([at, h, head, 1])
        return found

    runs = [runs_of(c) for c in range(chunks)]

    def query_sends(i):
        c, part = tiles[i]
        return [
            (
                not_me(z, u),
                pltpu.make_async_remote_copy(
                    src_ref=(qall.at[c, my_j] if u else qown.at[c]).at[:, part],
                    dst_ref=qall.at[c, my_j].at[:, part],
                    send_sem=qg_send,
                    recv_sem=qg_recv.at[i, my_j],
                    device_id=device(z, u),
                    device_id_type=MESH,
                ),
            )
            for u in (0, 1)
            for z in order
        ]

    @pl.when(owning)
    def _():
        for i in range(len(units) - 1):
            c, part = tiles[i]
            size = units[i + 1] - units[i]
            lo = units[i] + (i > 0)
            arrived = qrecv.at[pl.ds(0, 2 * n - 1), pl.ds(lo, size + (i == 0))]
            pltpu.make_async_copy(arrived, arrived, qs_recv.at[i]).wait()
            total = functools.reduce(jnp.add, [qrecv[2 * z + 1, squared] for z in range(n)])
            inv = lax.rsqrt(total / width + EPS) * (1.0 / HD**0.5)
            for h in (0, 1):
                planes = pl.ds(lo, size)
                q = functools.reduce(jnp.add, [qrecv[2 * z + h, planes] for z in range(n)])
                q = (q * inv[None]).astype(BF16).astype(F32)
                qturn[h * size : (h + 1) * size] = q
            for r in range(piece):
                qown[c, r, part] = qturn[: 2 * size, r, :]
                qall[c, my_j, r, part] = qturn[: 2 * size, piece + r, :]
            for go, copy in query_sends(i):
                pl.when(go)(copy.start)
            if units[i + 1] == hc:
                for k in range(1, m):
                    flip(k)

    lanes = lax.broadcasted_iota(jnp.int32, (full, HD), 1)
    lanes = lanes - lax.broadcasted_iota(jnp.int32, (full, HD), 0) * each
    positions = me * block + lax.broadcasted_iota(jnp.int32, (full, block), 1)

    def keep_own(c):
        for s in range(subs):
            arecv[c, s, 1, me] = asend[c, my_j, s]
            srecv[c, s, n + me] = ssend[c, my_j, s]

    def stats_send(c, j, s):
        return pltpu.make_async_remote_copy(
            src_ref=ssend.at[c, j, s],
            dst_ref=srecv.at[c, s, core * n + me],
            send_sem=ss_send,
            recv_sem=ss_recv.at[c, s],
            device_id=device(first + j, 1),
            device_id_type=MESH,
        )

    def result_send(c, j, s):
        return pltpu.make_async_remote_copy(
            src_ref=asend.at[c, j, s],
            dst_ref=arecv.at[c, s, core, me],
            send_sem=as_send,
            recv_sem=as_recv.at[c, s, core],
            device_id=device(first + j, 1),
            device_id_type=MESH,
        )

    adds = jnp.where(me == n // 2, 1.0, 0.0)

    for c in range(chunks):
        for k in range(m):
            j = lax.rem(my_j + m - 1 - k, m)
            for i, (chunk, part) in enumerate(tiles):
                if chunk == c:
                    arrival = pltpu.make_async_remote_copy(
                        src_ref=qall.at[c, j].at[:, part],
                        dst_ref=qall.at[c, j].at[:, part],
                        send_sem=qg_send,
                        recv_sem=qg_recv.at[i, j],
                        device_id=device(me, other),
                        device_id_type=MESH,
                    )
                    pl.when(not_me(first + j, 1))(arrival.wait_recv)
            scores, own = [], []
            for r in range(piece):
                q = qall[c, j, r]
                scores.append(
                    jnp.dot(q.astype(BF16), kturn[j * piece + r], preferred_element_type=F32)
                )
                row = core * half_rows + j * piece + r
                own.append(jnp.sum(q * newf[0, pl.ds(row, 1)], axis=-1, keepdims=True))
            if c == 0 and k == 0:
                later[1].wait()
            for s in range(subs):
                stats = jnp.zeros((full, HD), F32)
                for i in range(part_rows):
                    r = s * part_rows + i
                    row = core * half_rows + j * piece + r
                    live = positions < lens_ref[row]
                    masked = jnp.where(live, scores[r], -jnp.inf)
                    top = jnp.maximum(jnp.max(masked, axis=-1, keepdims=True), own[r])
                    weights = jnp.exp(masked - top)
                    fresh = jnp.exp(own[r] - top) * adds
                    weight = jnp.sum(weights, axis=-1, keepdims=True) + fresh
                    stats = jnp.where(lanes == 2 * i, top, stats)
                    stats = jnp.where(lanes == 2 * i + 1, weight, stats)
                    product = jnp.dot(
                        weights.astype(BF16), vbuf[j * piece + r], preferred_element_type=F32
                    )
                    product = product + fresh * newf[1, pl.ds(row, 1)]
                    asend[c, j, s, i * full : (i + 1) * full] = product
                ssend[c, j, s] = jnp.sum(stats, axis=0, keepdims=True)

            @pl.when(not_me(first + j, 1))
            def _(c=c, j=j):
                for s in range(subs):
                    stats_send(c, j, s).start()
                    result_send(c, j, s).start()

            pl.when(is_me(first + j, 1))(functools.partial(keep_own, c))

    def returns(c, s, u, stops):
        group = pl.ds(u * half_rows + my_j * piece + s * part_rows, part_rows)
        return [
            (
                not_me(z, h),
                pltpu.make_async_remote_copy(
                    src_ref=att.at[c, group] if h else aout.at[c, s, u],
                    dst_ref=att.at[c, group],
                    send_sem=ag_send,
                    recv_sem=ag_recv.at[c],
                    device_id=device(z, h),
                    device_id_type=MESH,
                ),
            )
            for z in stops
            for h in (0, 1)
        ]

    def share_out(c, s):
        arrived = srecv.at[c, s, pl.ds(0, 2 * n - 1)]
        pltpu.make_async_copy(arrived, arrived, ss_recv.at[c, s]).wait()
        for u in (1, 0):
            stats = [jnp.broadcast_to(srecv[c, s, u * n + z], (8, HD)) for z in range(n)]
            top = functools.reduce(jnp.maximum, stats)
            factors = [jnp.exp(line - top) for line in stats]
            totals = functools.reduce(
                jnp.add, [pltpu.roll(stats[z], HD - 1, 1) * factors[z] for z in range(n)]
            )
            inverse = 1.0 / totals
            for i in range(part_rows):
                for t in range(full // 8):
                    here = lanes[t * 8 : t * 8 + 8] == 2 * i
                    at = i * full + t * 8
                    for z, factor in enumerate(factors):
                        one = jnp.where(here, factor * inverse, 0.0)
                        one = jnp.sum(one, axis=-1, keepdims=True)
                        coef[u, z, at : at + 8] = jnp.broadcast_to(one, (8, HD))

    @pl.when(owning)
    def _():
        for c in range(chunks):
            for s in range(subs):
                last = c == chunks - 1 and s == subs - 1
                share_out(c, s)
                for u in (1, 0):
                    arrived = arecv.at[c, s, u, pl.ds(0, n - u)]
                    pltpu.make_async_copy(arrived, arrived, as_recv.at[c, s, u]).wait()
                    for i in range(part_rows):
                        row = u * half_rows + my_j * piece + s * part_rows + i
                        for t in range(full // 8):
                            at = slice(i * full + t * 8, i * full + t * 8 + 8)
                            result = functools.reduce(
                                jnp.add,
                                [coef[u, z, at] * arecv[c, s, u, z, at] for z in range(n)],
                            )
                            result = result.astype(BF16).astype(F32)
                            for at, h, head, size in runs[c][t]:
                                span_in = slice(at, at + size)
                                if h:
                                    att[c, row, head : head + size] = result[span_in]
                                else:
                                    aout[c, s, u, i, head : head + size] = result[span_in]
                    if not last:
                        ready = returns(c, s, u, order)
                    else:
                        ready = returns(c, s, u, order[:2])
                        if u == 0:
                            ready += returns(c, s, 1, order[2:]) + returns(c, s, 0, order[2:])
                    for go, copy in ready:
                        pl.when(go)(copy.start)

    sent, kept = None, None
    for c in range(chunks):
        for owner, count in ((owning, rows - share), (resting, rows)):
            arrived = att.at[c, pl.ds(0, count)]
            pl.when(owner)(pltpu.make_async_copy(arrived, arrived, ag_recv.at[c]).wait)
        if c == 0:
            pltpu.make_async_copy(wout, wout, wo_sem).wait()
        attended = jnp.concatenate([att[c, :, h, :] for h in range(hc)], axis=1).astype(BF16)
        deep = slice(c * hc * HD, (c + 1) * hc * HD)
        product = jnp.dot(attended, wout[0, deep], preferred_element_type=F32)
        sent = product if sent is None else sent + product
        if c == chunks - 1:
            hsend[...] = sent
            swap = pltpu.make_async_remote_copy(
                src_ref=hsend,
                dst_ref=hrecv,
                send_sem=h_sem.at[0],
                recv_sem=h_sem.at[1],
                device_id=device(me, other),
                device_id_type=MESH,
            )
            swap.start()
        product = jnp.dot(attended, wout[1, deep], preferred_element_type=F32)
        kept = product if kept is None else kept + product
    swap.wait_recv()
    out_ref[...] = kept + hrecv[...]
    swap.wait_send()

    def drain(ref, sem):
        pltpu.make_async_copy(ref, ref, sem).wait()

    @pl.when(resting)
    def _():
        drain(qsend, qs_send)
        drain(asend, as_send)
        drain(ssend, ss_send)

    @pl.when(owning)
    def _():
        drain(qsend.at[pl.ds(0, m - 1)], qs_send)
        drain(asend.at[:, pl.ds(0, m - 1)], as_send)
        drain(ssend.at[:, pl.ds(0, m - 1)], ss_send)
        drain(tally, qg_send)
        drain(tally, ag_send)


def solution(mesh):
    n = mesh.shape["seq"]
    m = max(n // 2, 2)

    def shards(hidden, gain, wq, keys, values, knew, vnew, lengths, wout):
        rows, depth = hidden.shape
        heads = wq.shape[1] // HD
        share = rows // m
        piece = share // 2
        subs = 1
        units = tuple(heads * e // UNITS[-1] for e in UNITS)
        block = keys.shape[1]
        half = wout.shape[1] // 2
        hc = heads // CHUNKS
        cuts = tuple(heads * e // EDGES[-1] for e in EDGES)
        anywhere = pl.BlockSpec(memory_space=pl.ANY)
        dma = pltpu.SemaphoreType.DMA
        return pl.pallas_call(
            functools.partial(kernel, n, heads, rows, m, cuts, CHUNKS, units),
            out_shape=pltpu.VMEM((rows, half), F32),
            in_specs=[anywhere] * 9,
            out_specs=pl.BlockSpec(memory_space=pltpu.VMEM),
            scratch_shapes=[
                pltpu.SMEM((rows,), jnp.int32),
                pltpu.VMEM((rows, depth), BF16),
                pltpu.VMEM((depth // HD, HD), BF16),
                pltpu.VMEM(wq.shape, BF16),
                pltpu.VMEM((rows // 2, block, HD), BF16),
                pltpu.VMEM((rows // 2, block, HD), BF16),
                pltpu.VMEM((2, rows, HD), BF16),
                pltpu.VMEM((2, wout.shape[0], half), BF16),
                pltpu.VMEM((2, rows, HD), F32),
                pltpu.VMEM((m, heads + 1, share, HD), F32),
                pltpu.VMEM((2 * n, heads + 1, share, HD), F32),
                pltpu.VMEM((2 * hc, share, HD), F32),
                pltpu.VMEM((CHUNKS, piece, 2 * hc, HD), F32),
                pltpu.VMEM((CHUNKS, m, piece, 2 * hc, HD), F32),
                pltpu.VMEM((rows // 2, HD, block), BF16),
                pltpu.VMEM((CHUNKS, m, subs, 1, HD), F32),
                pltpu.VMEM((CHUNKS, subs, 2 * n, 1, HD), F32),
                pltpu.VMEM((2, n, piece // subs * 2 * hc, HD), F32),
                pltpu.VMEM((CHUNKS, m, subs, piece // subs * 2 * hc, HD), F32),
                pltpu.VMEM((CHUNKS, subs, 2, n, piece // subs * 2 * hc, HD), F32),
                pltpu.VMEM((CHUNKS, subs, 2, piece // subs, hc, HD), F32),
                pltpu.VMEM((CHUNKS, rows, hc, HD), F32),
                pltpu.VMEM((rows, half), F32),
                pltpu.VMEM((rows, half), F32),
                pltpu.VMEM((CHUNKS, 2 * n - 1, piece, 2 * hc, HD), F32),
                dma((4,)),
                dma((len(cuts) - 1,)),
                dma((2,)),
                dma(()),
                dma(()),
                dma((len(units) - 1,)),
                dma(()),
                dma((len(units) - 1, m)),
                dma(()),
                dma((CHUNKS, subs)),
                dma(()),
                dma((CHUNKS, subs, 2)),
                dma(()),
                dma((CHUNKS,)),
                dma((2,)),
            ],
            compiler_params=pltpu.CompilerParams(collective_id=0, has_side_effects=True),
            name="decode_step",
        )(lengths, hidden, gain.reshape(-1, HD), wq, keys, values, knew, vnew, wout)

    placed = (
        P(("groups", "batch"), "seq"),
        P("seq"),
        P("seq", "head"),
        P(("groups", "batch"), "seq", None),
        P(("groups", "batch"), "seq", None),
        P(("groups", "batch"), None),
        P(("groups", "batch"), None),
        P(("groups", "batch")),
        P("head", "seq"),
    )
    return jax.shard_map(
        shards,
        mesh=mesh,
        in_specs=placed,
        out_specs=P(("groups", "batch"), ("seq", "head")),
        check_vma=False,
    )
```
